32 devices in a mesh: dp: 4 (over y, z), ep: 8 (over x, core).
Axes of the slice: x: 4, y: 2, z: 2, core: 2. Of those that a mesh axis runs over, the one named last changes fastest.
The devices are a block of a 4x4x8 slice.
Arguments:
- tokens: bfloat16 [64, 256, 1024], P(('dp', 'ep')), parts along dimension 0
- attn_gain_1: bfloat16 [1024], replicated
- w_query_1: bfloat16 [1024, 8, 128], replicated
- w_key_1: bfloat16 [1024, 2, 128], replicated
- w_value_1: bfloat16 [1024, 2, 128], replicated
- w_out_1: bfloat16 [8, 128, 1024], replicated
- moe_gain_1: bfloat16 [1024], replicated
- w_router_1: bfloat16 [1024, 16], replicated
- routes_1: int32 [64, 256, 4], P(('dp', 'ep')), parts along dimension 0
- w_gate_1: bfloat16 [16, 1024, 1792], P('ep')
- w_up_1: bfloat16 [16, 1024, 1792], P('ep')
- w_down_1: bfloat16 [16, 1792, 1024], P('ep')
- shared_gate_1: bfloat16 [1024, 1792], replicated
- shared_up_1: bfloat16 [1024, 1792], replicated
- shared_down_1: bfloat16 [1792, 1024], replicated
- attn_gain_2: bfloat16 [1024], replicated
- w_query_2: bfloat16 [1024, 8, 128], replicated
- w_key_2: bfloat16 [1024, 2, 128], replicated
- w_value_2: bfloat16 [1024, 2, 128], replicated
- w_out_2: bfloat16 [8, 128, 1024], replicated
- moe_gain_2: bfloat16 [1024], replicated
- w_router_2: bfloat16 [1024, 16], replicated
- routes_2: int32 [64, 256, 4], P(('dp', 'ep')), parts along dimension 0
- w_gate_2: bfloat16 [16, 1024, 1792], P('ep')
- w_up_2: bfloat16 [16, 1024, 1792], P('ep')
- w_down_2: bfloat16 [16, 1792, 1024], P('ep')
- shared_gate_2: bfloat16 [1024, 1792], replicated
- shared_up_2: bfloat16 [1024, 1792], replicated
- shared_down_2: bfloat16 [1792, 1024], replicated
Outputs:
- output: bfloat16 [64, 256, 1024], P(('dp', 'ep')), parts along dimension 0
There are 4 independent parts. The reference program is written for one: setup_inputs(seed, part) draws one part's arguments, and reference() takes and returns one part's arrays. A program takes and returns all parts, laid end to end along the dimension named above; an argument that names none is the same for every part.
All inputs are finite; a program needn't handle non-finite values.
Results may differ from the reference program's by a relative error of at most 0.02.
Values are sent between devices in bfloat16 or wider.
A program may use at most 768 MiB of HBM per device.

```python
import jax
import jax.numpy as jnp
from jax import lax

EP_SIZE = 8
SEQS_DEV = 2
SEQ_LEN = 256
MODEL_DIM = 1024
NUM_EXPERTS = 16
TOP_K = 4
EXPERT_FF = 1792
SHARED_FF = 1792
QUERY_HEADS = 8
KV_HEADS = 2
HEAD_DIM = 128

TOKENS_DEV = SEQS_DEV * SEQ_LEN
HALF_TOKENS = TOKENS_DEV // 2
MEAN_ROWS = HALF_TOKENS * TOP_K // NUM_EXPERTS
CAPACITY = 6 * MEAN_ROWS
GROUP_SIZE = QUERY_HEADS // KV_HEADS
NORM_EPS = 1e-6
LAYER_NAMES = ('attn_gain', 'w_query', 'w_key', 'w_value', 'w_out', 'moe_gain', 'w_router', 'routes', 'w_gate', 'w_up', 'w_down', 'shared_gate', 'shared_up', 'shared_down')


def draw_routes(key):
    dev_key, row_key = jax.random.split(key)
    dev_order = jax.random.permutation(dev_key, EP_SIZE)
    level_units = jnp.array([12, 2, 1, 1], dtype=jnp.int32)
    dev_level = level_units[dev_order % 4]
    expert_counts = jnp.repeat(dev_level, NUM_EXPERTS // EP_SIZE) * (MEAN_ROWS // 4)
    expert_list = jnp.repeat(jnp.arange(NUM_EXPERTS, dtype=jnp.int32), expert_counts, total_repeat_length=HALF_TOKENS * TOP_K)
    base_grid = expert_list.reshape(TOP_K, HALF_TOKENS).T

    def one_half(sub_key):
        perm_key, shift_key = jax.random.split(sub_key)
        tok_order = jax.random.permutation(perm_key, HALF_TOKENS)
        shift = jax.random.randint(shift_key, (HALF_TOKENS, 1), 0, TOP_K)
        slot_order = (jnp.arange(TOP_K)[None, :] + shift) % TOP_K
        return jnp.take_along_axis(base_grid[tok_order], slot_order, axis=1)

    halves = jax.vmap(one_half)(jax.random.split(row_key, 2 * EP_SIZE))
    return halves.reshape(EP_SIZE * SEQS_DEV, SEQ_LEN, TOP_K).astype(jnp.int32)


def normal_weight(key, shape, scale):
    return (jax.random.normal(key, shape, jnp.float32) * scale).astype(jnp.bfloat16)


def draw_gain(key):
    return jax.random.uniform(key, (MODEL_DIM,), jnp.float32, 0.6, 1.4).astype(jnp.bfloat16)


def draw_layer(keys, route_key):
    return (
        draw_gain(keys[0]),
        normal_weight(keys[1], (MODEL_DIM, QUERY_HEADS, HEAD_DIM), 1.2 * MODEL_DIM ** -0.5),
        normal_weight(keys[2], (MODEL_DIM, KV_HEADS, HEAD_DIM), 1.2 * MODEL_DIM ** -0.5),
        normal_weight(keys[3], (MODEL_DIM, KV_HEADS, HEAD_DIM), MODEL_DIM ** -0.5),
        normal_weight(keys[4], (QUERY_HEADS, HEAD_DIM, MODEL_DIM), 2.0 * (QUERY_HEADS * HEAD_DIM) ** -0.5),
        draw_gain(keys[5]),
        normal_weight(keys[6], (MODEL_DIM, NUM_EXPERTS), 1.5 * MODEL_DIM ** -0.5),
        draw_routes(route_key),
        normal_weight(keys[7], (NUM_EXPERTS, MODEL_DIM, EXPERT_FF), MODEL_DIM ** -0.5),
        normal_weight(keys[8], (NUM_EXPERTS, MODEL_DIM, EXPERT_FF), MODEL_DIM ** -0.5),
        normal_weight(keys[9], (NUM_EXPERTS, EXPERT_FF, MODEL_DIM), 1.5 * EXPERT_FF ** -0.5),
        normal_weight(keys[10], (MODEL_DIM, SHARED_FF), MODEL_DIM ** -0.5),
        normal_weight(keys[11], (MODEL_DIM, SHARED_FF), MODEL_DIM ** -0.5),
        normal_weight(keys[12], (SHARED_FF, MODEL_DIM), 0.8 * SHARED_FF ** -0.5),
    )


def setup_inputs(seed: int = 0, part: int = 0) -> dict:
    base_key = jax.random.key(seed)
    part_key = jax.random.fold_in(base_key, part)
    weight_keys = jax.random.split(base_key, 26)
    data_keys = jax.random.split(part_key, 3)
    inputs = {'tokens': jax.random.normal(data_keys[0], (EP_SIZE * SEQS_DEV, SEQ_LEN, MODEL_DIM), jnp.float32).astype(jnp.bfloat16)}
    layer_one = draw_layer(weight_keys[:13], data_keys[1])
    layer_two = draw_layer(weight_keys[13:], data_keys[2])
    for name, value in zip(LAYER_NAMES, layer_one):
        inputs[name + '_1'] = value
    for name, value in zip(LAYER_NAMES, layer_two):
        inputs[name + '_2'] = value
    return inputs


def rms_norm(hidden, gain):
    hidden_f32 = hidden.astype(jnp.float32)
    inv_rms = lax.rsqrt(jnp.mean(hidden_f32 * hidden_f32, axis=-1, keepdims=True) + NORM_EPS)
    return (hidden_f32 * inv_rms * gain.astype(jnp.float32)).astype(jnp.bfloat16)


def attention_block(hidden, gain, w_query, w_key, w_value, w_out):
    normed = rms_norm(hidden, gain).astype(jnp.float32)
    query = jnp.einsum('bsd,dnh->bsnh', normed, w_query.astype(jnp.float32)).astype(jnp.bfloat16)
    query = query.reshape(SEQS_DEV, SEQ_LEN, KV_HEADS, GROUP_SIZE, HEAD_DIM).astype(jnp.float32)
    key_proj = jnp.einsum('bsd,dkh->bskh', normed, w_key.astype(jnp.float32)).astype(jnp.bfloat16).astype(jnp.float32)
    value = jnp.einsum('bsd,dkh->bskh', normed, w_value.astype(jnp.float32)).astype(jnp.bfloat16).astype(jnp.float32)
    scores = jnp.einsum('bskgh,btkh->bkgst', query, key_proj) * HEAD_DIM ** -0.5
    causal = jnp.arange(SEQ_LEN)[:, None] >= jnp.arange(SEQ_LEN)[None, :]
    attn_probs = jax.nn.softmax(jnp.where(causal, scores, -1e30), axis=-1).astype(jnp.bfloat16).astype(jnp.float32)
    mixed = jnp.einsum('bkgst,btkh->bskgh', attn_probs, value).astype(jnp.bfloat16).astype(jnp.float32)
    out_heads = w_out.astype(jnp.float32).reshape(KV_HEADS, GROUP_SIZE, HEAD_DIM, MODEL_DIM)
    projected = jnp.einsum('bskgh,kghd->bsd', mixed, out_heads)
    return (hidden.astype(jnp.float32) + projected).astype(jnp.bfloat16)


def dispatch_plan(choices):
    num_rows = TOKENS_DEV * TOP_K
    flat_ids = choices.reshape(num_rows)
    order = jnp.argsort(flat_ids, stable=True)
    sorted_ids = flat_ids[order]
    expert_ids = jnp.arange(NUM_EXPERTS, dtype=flat_ids.dtype)
    starts = jnp.searchsorted(sorted_ids, expert_ids, side='left')
    ends = jnp.searchsorted(sorted_ids, expert_ids, side='right')
    slot_src = starts[:, None] + jnp.arange(CAPACITY)[None, :]
    slot_used = slot_src < ends[:, None]
    slot_token = order[jnp.minimum(slot_src, num_rows - 1)] // TOP_K
    rank = jnp.zeros((num_rows,), order.dtype).at[order].set(jnp.arange(num_rows, dtype=order.dtype))
    row_loc = flat_ids * CAPACITY + rank - starts[flat_ids]
    return slot_token, slot_used, row_loc.reshape(TOKENS_DEV, TOP_K)


def moe_layer(hidden, choices, params):
    (attn_gain, w_query, w_key, w_value, w_out, moe_gain, w_router, w_gate, w_up, w_down, shared_gate, shared_up, shared_down) = params
    residual = attention_block(hidden, attn_gain, w_query, w_key, w_value, w_out).reshape(TOKENS_DEV, MODEL_DIM)
    normed = rms_norm(residual, moe_gain)
    logits = jnp.dot(normed, w_router, preferred_element_type=jnp.float32)
    gates = jax.nn.softmax(jnp.take_along_axis(logits, choices, axis=1), axis=-1)
    slot_token, slot_used, row_loc = dispatch_plan(choices)
    rows = jnp.where(slot_used[:, :, None], normed[slot_token], jnp.zeros((), jnp.bfloat16)).astype(jnp.float32)
    gate_act = jnp.einsum('ecd,edf->ecf', rows, w_gate)
    up_act = jnp.einsum('ecd,edf->ecf', rows, w_up)
    hidden_act = (jax.nn.silu(gate_act) * up_act).astype(jnp.bfloat16).astype(jnp.float32)
    expert_out = jnp.einsum('ecf,efd->ecd', hidden_act, w_down).astype(jnp.bfloat16)
    picked = expert_out.reshape(NUM_EXPERTS * CAPACITY, MODEL_DIM)[row_loc].astype(jnp.float32)
    routed = jnp.sum(gates[:, :, None] * picked, axis=1)
    shared_gate_act = jnp.dot(normed, shared_gate, preferred_element_type=jnp.float32)
    shared_up_act = jnp.dot(normed, shared_up, preferred_element_type=jnp.float32)
    shared_hidden = (jax.nn.silu(shared_gate_act) * shared_up_act).astype(jnp.bfloat16)
    shared = jnp.dot(shared_hidden, shared_down, preferred_element_type=jnp.float32)
    layer_out = (residual.astype(jnp.float32) + routed + shared).astype(jnp.bfloat16)
    return layer_out.reshape(SEQS_DEV, SEQ_LEN, MODEL_DIM)


def reference(tokens, attn_gain_1, w_query_1, w_key_1, w_value_1, w_out_1, moe_gain_1, w_router_1, routes_1, w_gate_1, w_up_1, w_down_1, shared_gate_1, shared_up_1, shared_down_1, attn_gain_2, w_query_2, w_key_2, w_value_2, w_out_2, moe_gain_2, w_router_2, routes_2, w_gate_2, w_up_2, w_down_2, shared_gate_2, shared_up_2, shared_down_2):
    params_one = (attn_gain_1, w_query_1, w_key_1, w_value_1, w_out_1, moe_gain_1, w_router_1, w_gate_1.astype(jnp.float32), w_up_1.astype(jnp.float32), w_down_1.astype(jnp.float32), shared_gate_1, shared_up_1, shared_down_1)
    params_two = (attn_gain_2, w_query_2, w_key_2, w_value_2, w_out_2, moe_gain_2, w_router_2, w_gate_2.astype(jnp.float32), w_up_2.astype(jnp.float32), w_down_2.astype(jnp.float32), shared_gate_2, shared_up_2, shared_down_2)

    def one_source(block):
        hidden, route_one, route_two = block
        hidden = moe_layer(hidden, route_one, params_one)
        return moe_layer(hidden, route_two, params_two)

    blocks = (tokens.reshape(EP_SIZE, SEQS_DEV, SEQ_LEN, MODEL_DIM), routes_1.reshape(EP_SIZE, TOKENS_DEV, TOP_K), routes_2.reshape(EP_SIZE, TOKENS_DEV, TOP_K))
    return lax.map(one_source, blocks).reshape(EP_SIZE * SEQS_DEV, SEQ_LEN, MODEL_DIM)
```

```python
import functools

import jax
import jax.numpy as jnp
from jax import lax
from jax.experimental import pallas as pl
from jax.experimental.pallas import tpu as pltpu
from jax.sharding import PartitionSpec as P

NORM_EPS = 1e-6
MESH = pl.DeviceIdType.MESH
F32 = jnp.float32
BF16 = jnp.bfloat16

OWN0, OPP0, OPP1, LEFT1, RIGHT0, LEFT0, RIGHT1, OWN1 = range(8)
UNITS = 8
CHUNK = 256


def rms_norm(hidden, gain):
    hidden_f32 = hidden.astype(F32)
    inv_rms = lax.rsqrt(jnp.mean(hidden_f32 * hidden_f32, axis=-1, keepdims=True) + NORM_EPS)
    return (hidden_f32 * inv_rms * gain.astype(F32)).astype(BF16)


def attention_block(hidden, gain, w_query, w_key, w_value, w_out):
    batch, seq_len, model_dim = hidden.shape
    heads, head_dim = w_query.shape[1], w_query.shape[2]
    kv_heads = w_key.shape[1]
    group = heads // kv_heads
    normed = rms_norm(hidden, gain)
    query = jnp.einsum('bsd,dnh->bsnh', normed, w_query, preferred_element_type=F32).astype(BF16)
    query = query.reshape(batch, seq_len, kv_heads, group, head_dim)
    key_proj = jnp.einsum('bsd,dkh->bskh', normed, w_key, preferred_element_type=F32).astype(BF16)
    value = jnp.einsum('bsd,dkh->bskh', normed, w_value, preferred_element_type=F32).astype(BF16)
    scores = jnp.einsum('bskgh,btkh->bkgst', query, key_proj, preferred_element_type=F32) * (head_dim ** -0.5)
    causal = lax.broadcasted_iota(jnp.int32, (seq_len, seq_len), 0) >= lax.broadcasted_iota(jnp.int32, (seq_len, seq_len), 1)
    attn_probs = jax.nn.softmax(jnp.where(causal, scores, -1e30), axis=-1).astype(BF16)
    mixed = jnp.einsum('bkgst,btkh->bskgh', attn_probs, value, preferred_element_type=F32).astype(BF16)
    out_heads = w_out.reshape(kv_heads, group, head_dim, model_dim)
    projected = jnp.einsum('bskgh,kghd->bsd', mixed, out_heads, preferred_element_type=F32)
    return (hidden.astype(F32) + projected).astype(BF16)


def routing_rows(normed, w_router, routes, ep_size, local_count):
    halves, half_len, model_dim = normed.shape
    num_experts = w_router.shape[1]
    logits = jnp.einsum('htd,de->het', normed, w_router, preferred_element_type=F32)
    experts = lax.broadcasted_iota(jnp.int32, (1, num_experts, 1, 1), 1)
    chosen = jnp.any(jnp.swapaxes(routes, 1, 2)[:, None, :, :] == experts, axis=2)
    masked = jnp.where(chosen, logits, -jnp.inf)
    weights = jnp.exp(masked - jnp.max(masked, axis=1, keepdims=True))
    gates = weights / jnp.sum(weights, axis=1, keepdims=True)
    before = (lax.broadcasted_iota(jnp.int32, (half_len, half_len), 0) < lax.broadcasted_iota(jnp.int32, (half_len, half_len), 1)).astype(BF16)
    place = jnp.einsum('het,ts->hes', chosen.astype(BF16), before, preferred_element_type=F32)
    place = jnp.where(chosen, place, -1.0)
    gates = gates.reshape(halves, ep_size, local_count, half_len)
    place = place.reshape(halves, ep_size, local_count, half_len)
    pad = jnp.zeros((halves, ep_size, 8 - 2 * local_count, half_len), F32)
    return jnp.swapaxes(jnp.concatenate([gates, place, pad], axis=2), 0, 1)


def moe_kernel(
    ep_size, rows_half,
    u_ref, meta_ref, res_ref, wg_ref, wu_ref, wd_ref, sg_ref, su_ref, sd_ref, out_ref,
    ub, mb, wg, wu, wd, sg, su, sd, acc, xb, hb, yb, keep, dsend, drecv, isend, rbuf,
    wsem, shsem, lsem, fs, fr, uss, urs, mss, mrs, dss, drs, iss, irs, credit,
):
    chips = ep_size // 2
    me = lax.axis_index('ep')
    chip, core = me // 2, me % 2
    other = 1 - core
    sib = 2 * chip + other
    left = 2 * ((chip + chips - 1) % chips) + core
    right = 2 * ((chip + 1) % chips) + core
    ff = wg.shape[2]
    model_dim = wg.shape[1]
    half_len = ub.shape[2]
    n_ff, n_out = ff // CHUNK, model_dim // CHUNK

    def remote(src, dst, send, recv, device):
        return pltpu.make_async_remote_copy(src_ref=src, dst_ref=dst, send_sem=send, recv_sem=recv, device_id={'ep': device}, device_id_type=MESH)

    def shared_piece(j, slot):
        cols = pl.ds(pl.multiple_of(j * CHUNK, CHUNK), CHUNK)
        return (
            pltpu.make_async_copy(sg_ref.at[:, cols], sg.at[slot], shsem.at[slot, 0]),
            pltpu.make_async_copy(su_ref.at[:, cols], su.at[slot], shsem.at[slot, 1]),
            pltpu.make_async_copy(sd_ref.at[cols, :], sd.at[slot], shsem.at[slot, 2]),
        )

    def expert_weights(e):
        return (
            pltpu.make_async_copy(wg_ref.at[e], wg.at[e], wsem.at[e, 0]),
            pltpu.make_async_copy(wu_ref.at[e], wu.at[e], wsem.at[e, 1]),
            pltpu.make_async_copy(wd_ref.at[e], wd.at[e], wsem.at[e, 2]),
        )

    own_u = [pltpu.make_async_copy(u_ref.at[h], ub.at[slot, core], lsem.at[h]) for h, slot in ((0, OWN0), (1, OWN1))]
    own_m = [pltpu.make_async_copy(meta_ref.at[me, h], mb.at[slot, core], lsem.at[2 + h]) for h, slot in ((0, OWN0), (1, OWN1))]
    for copy in own_u:
        copy.start()
    for copy in own_m:
        copy.start()
    for copy in shared_piece(0, 0):
        copy.start()

    barrier = pltpu.get_barrier_semaphore()
    for step in range(1, ep_size):
        pl.semaphore_signal(barrier, inc=1, device_id={'ep': (me + step) % ep_size}, device_id_type=MESH)
    pl.semaphore_wait(barrier, ep_size - 1)

    def ring_u(src, slot, device):
        return remote(src, ub.at[slot, core], uss.at[slot], urs.at[slot], device)

    def partner_u(src, slot):
        return remote(src, ub.at[slot, core], fs.at[slot], fr.at[slot], sib)

    def partner_in(slot):
        return remote(ub.at[slot, other], ub.at[slot, other], fs.at[slot], fr.at[slot], sib)

    ring_u(u_ref.at[0], LEFT0, right).start()
    ring_u(u_ref.at[1], RIGHT1, left).start()
    partner_u(u_ref.at[0], OWN0).start()
    partner_u(u_ref.at[1], OWN1).start()

    meta_sends = []
    for hop, slots in ((0, (OWN0, OWN1)), (1, (LEFT0, LEFT1)), (2, (OPP0, OPP1)), (3, (RIGHT0, RIGHT1))):
        for flip in range(2):
            if hop == 0 and flip == 0:
                continue
            dest = 2 * ((chip + hop) % chips) + (core + flip) % 2
            for h, slot in enumerate(slots):
                meta_sends.append(remote(meta_ref.at[dest, h], mb.at[slot, core], mss.at[slot, flip], mrs.at[slot, core], dest))
    for copy in meta_sends:
        copy.start()

    for e in range(2):
        for copy in expert_weights(e):
            copy.start()
    for copy in own_u:
        copy.wait()
    for copy in own_m:
        copy.wait()

    for h in range(2):
        acc[h] = res_ref[h].astype(F32)

    def shared_step(j, carry):
        slot = j % 2

        @pl.when(j + 1 < n_ff)
        def _():
            for copy in shared_piece(j + 1, (j + 1) % 2):
                copy.start()

        for copy in shared_piece(j, slot):
            copy.wait()
        for h, own in ((0, OWN0), (1, OWN1)):
            rows = ub[own, core]
            gate_act = jnp.dot(rows, sg[slot], preferred_element_type=F32)
            up_act = jnp.dot(rows, su[slot], preferred_element_type=F32)
            act = (jax.nn.silu(gate_act) * up_act).astype(BF16)
            acc[h] += jnp.dot(act, sd[slot], preferred_element_type=F32)
        return carry

    lax.fori_loop(0, n_ff, shared_step, 0)

    def partial_copy(n):
        return remote(dsend.at[n % 2], drecv.at[n % 2], dss.at[n], drs.at[n], sib)

    def ring_copy(n):
        device = 2 * ((chip + 1 + (chips - 2) * (n % 2)) % chips) + core
        return remote(isend.at[n - 1], rbuf.at[n - 1], iss.at[n], irs.at[n], device)

    def merge(n):
        slot = n % 2
        partial_copy(n).wait_recv()

        @pl.when(jnp.logical_or(n == OWN0, n == OWN1))
        def _():
            acc[n // (UNITS - 1)] += keep[slot] + drecv[slot]

        @pl.when(jnp.logical_and(n != OWN0, n < LEFT0))
        def _():
            isend[n - 1] = keep[slot] + drecv[slot]

        for unit in (LEFT0, RIGHT1):
            @pl.when(n == unit)
            def _():
                ring_copy(unit - LEFT0 + OPP0).wait_recv()
                isend[unit - 1] = keep[slot] + drecv[slot] + rbuf[unit - LEFT0]

        @pl.when(n + 2 < UNITS)
        def _():
            pl.semaphore_signal(credit.at[slot], inc=1, device_id={'ep': sib}, device_id_type=MESH)

        @pl.when(jnp.logical_and(n != OWN0, n != OWN1))
        def _():
            ring_copy(n).start()

    def unit_step(n, carry):
        @pl.when(n == OPP0)
        def _():
            for slot in (OPP0, OPP1):
                ring_u(ub.at[slot, core], slot, left).wait_recv()
                partner_u(ub.at[slot, core], slot).start()

        partner_in(n).wait_recv()
        for part, kk in ((0, other), (1, core)):
            @pl.when(jnp.logical_or(jnp.logical_and(n != OWN0, n != OWN1), kk != core))
            def _():
                remote(mb.at[n, kk], mb.at[n, kk], mss.at[n, 0], mrs.at[n, kk], sib).wait_recv()

        for part, kk in ((0, other), (1, core)):
            rows = ub[n, kk]
            for e in range(2):
                place = mb[n, kk, 2 + e:3 + e, :].astype(jnp.int32)
                pick = (place == lax.broadcasted_iota(jnp.int32, (rows_half, half_len), 0)).astype(BF16)
                xb[e, part * rows_half:(part + 1) * rows_half, :] = jnp.dot(pick, rows, preferred_element_type=F32).astype(BF16)

        def expert_step(e, carry):
            @pl.when(n == OWN0)
            def _():
                for copy in expert_weights(e):
                    copy.wait()

            @pl.when(jnp.logical_and(n == OWN0, e == 1))
            def _():
                for slot, opp, device, own in ((LEFT0, OPP0, right, 1), (RIGHT1, OPP1, left, 0)):
                    ring_u(ub.at[slot, core], slot, device).wait_recv()
                    ring_u(ub.at[slot, core], opp, device).start()
                    ring_u(u_ref.at[own], LEFT1 if own == 1 else RIGHT0, device).start()
                    partner_u(ub.at[slot, core], slot).start()

            @pl.when(jnp.logical_and(n == OPP1, e == 1))
            def _():
                for slot, device in ((LEFT1, right), (RIGHT0, left)):
                    ring_u(ub.at[slot, core], slot, device).wait_recv()
                    partner_u(ub.at[slot, core], slot).start()

            rows = xb[e]

            def up_step(j, carry):
                cols = pl.ds(pl.multiple_of(j * CHUNK, CHUNK), CHUNK)
                gate_act = jnp.dot(rows, wg[e, :, cols], preferred_element_type=F32)
                up_act = jnp.dot(rows, wu[e, :, cols], preferred_element_type=F32)
                hb[:, cols] = (jax.nn.silu(gate_act) * up_act).astype(BF16)
                return carry

            lax.fori_loop(0, n_ff, up_step, 0)

            @pl.when(jnp.logical_and(n > 0, e == 0))
            def _():
                merge(n - 1)

            def down_step(j, carry):
                cols = pl.ds(pl.multiple_of(j * CHUNK, CHUNK), CHUNK)
                yb[e, :, cols] = jnp.dot(hb[...], wd[e, :, cols], preferred_element_type=F32).astype(BF16)
                return carry

            lax.fori_loop(0, n_out, down_step, 0)
            return carry

        lax.fori_loop(0, 2, expert_step, 0)

        @pl.when(n >= 2)
        def _():
            partial_copy(n - 2).wait_send()
            pl.semaphore_wait(credit.at[n % 2], 1)

        for part, kk in ((0, other), (1, core)):
            columns = jnp.transpose(mb[n, kk])
            picks = []
            for e in range(2):
                place = columns[:, 2 + e:3 + e].astype(jnp.int32)
                picks.append((place == lax.broadcasted_iota(jnp.int32, (half_len, rows_half), 1)).astype(BF16))
            target = dsend if part == 0 else keep

            for j in range(n_out):
                cols = pl.ds(j * CHUNK, CHUNK)
                total = None
                for e in range(2):
                    chosen = jnp.dot(picks[e], yb[e, part * rows_half:(part + 1) * rows_half, cols], preferred_element_type=F32)
                    term = columns[:, e:e + 1] * chosen
                    total = term if total is None else total + term
                target[n % 2, :, cols] = total
        partial_copy(n).start()
        return carry

    lax.fori_loop(0, UNITS, unit_step, 0)
    merge(UNITS - 1)

    for h, slots in ((0, (RIGHT0, LEFT0)), (1, (LEFT1, RIGHT1))):
        for slot in slots:
            ring_copy(slot).wait_recv()
        out_ref[h] = (acc[h] + rbuf[slots[0] - 1] + rbuf[slots[1] - 1]).astype(BF16)

    for slot in (OPP0, OPP1, LEFT1, RIGHT0, LEFT0, RIGHT1):
        ring_u(ub.at[slot, core], slot, right).wait_send()
        ring_copy(slot).wait_send()
    for slot in range(UNITS):
        partner_u(ub.at[slot, core], slot).wait_send()
    for copy in meta_sends:
        copy.wait_send()
    for n in (UNITS - 2, UNITS - 1):
        partial_copy(n).wait_send()


def moe_layer(u, meta, residual, w_gate, w_up, w_down, shared_gate, shared_up, shared_down, ep_size, rows_half, layer):
    halves, half_len, model_dim = u.shape
    ff = w_gate.shape[2]
    anyspec = pl.BlockSpec(memory_space=pl.ANY)
    vmem = pl.BlockSpec(memory_space=pltpu.VMEM)
    block = (half_len, model_dim)
    dma = pltpu.SemaphoreType.DMA
    return pl.pallas_call(
        functools.partial(moe_kernel, ep_size, rows_half),
        out_shape=jax.ShapeDtypeStruct(u.shape, BF16),
        in_specs=[anyspec, anyspec, vmem, anyspec, anyspec, anyspec, anyspec, anyspec, anyspec],
        out_specs=vmem,
        scratch_shapes=[
            pltpu.VMEM((UNITS, 2) + block, BF16),
            pltpu.VMEM((UNITS, 2, 8, half_len), F32),
            pltpu.VMEM((2, model_dim, ff), BF16),
            pltpu.VMEM((2, model_dim, ff), BF16),
            pltpu.VMEM((2, ff, model_dim), BF16),
            pltpu.VMEM((2, model_dim, CHUNK), BF16),
            pltpu.VMEM((2, model_dim, CHUNK), BF16),
            pltpu.VMEM((2, CHUNK, model_dim), BF16),
            pltpu.VMEM((2,) + block, F32),
            pltpu.VMEM((2, 2 * rows_half, model_dim), BF16),
            pltpu.VMEM((2 * rows_half, ff), BF16),
            pltpu.VMEM((2, 2 * rows_half, model_dim), BF16),
            pltpu.VMEM((2,) + block, F32),
            pltpu.VMEM((2,) + block, F32),
            pltpu.VMEM((2,) + block, F32),
            pltpu.VMEM((6,) + block, F32),
            pltpu.VMEM((6,) + block, F32),
            dma((2, 3)), dma((2, 3)), dma((4,)),
            dma((UNITS,)), dma((UNITS,)), dma((UNITS,)), dma((UNITS,)),
            dma((UNITS, 2)), dma((UNITS, 2)),
            dma((UNITS,)), dma((UNITS,)), dma((UNITS,)), dma((UNITS,)),
            pltpu.SemaphoreType.REGULAR((2,)),
        ],
        compiler_params=pltpu.CompilerParams(collective_id=layer, has_side_effects=True, vmem_limit_bytes=67043328),
        name='moe_layer',
    )(u, meta, residual, w_gate, w_up, w_down, shared_gate, shared_up, shared_down)


def layer_step(hidden, layer_params, ep_size, layer):
    (attn_gain, w_query, w_key, w_value, w_out, moe_gain, w_router, routes, w_gate, w_up, w_down, shared_gate, shared_up, shared_down) = layer_params
    batch, seq_len, model_dim = hidden.shape
    local_count = w_gate.shape[0]
    num_experts = local_count * ep_size
    rows_half = 3 * seq_len * routes.shape[-1] // num_experts
    residual = attention_block(hidden, attn_gain, w_query, w_key, w_value, w_out)
    normed = rms_norm(residual, moe_gain)
    meta = routing_rows(normed, w_router, routes, ep_size, local_count)
    return moe_layer(normed, meta, residual, w_gate, w_up, w_down, shared_gate, shared_up, shared_down, ep_size, rows_half, layer)


def solution(mesh):
    ep_size = mesh.shape['ep']
    token_spec = P(('dp', 'ep'))
    layer_specs = (P(), P(), P(), P(), P(), P(), P(), token_spec, P('ep'), P('ep'), P('ep'), P(), P(), P())
    in_specs = (token_spec,) + layer_specs + layer_specs

    def local_step(tokens, *params):
        hidden = tokens
        for layer in range(2):
            hidden = layer_step(hidden, params[14 * layer:14 * layer + 14], ep_size, layer)
        return hidden

    return jax.shard_map(local_step, mesh=mesh, in_specs=in_specs, out_specs=token_spec, check_vma=False)
```

```python
import functools

import jax
import jax.numpy as jnp
from jax import lax
from jax.experimental import pallas as pl
from jax.experimental.pallas import tpu as pltpu
from jax.sharding import PartitionSpec as P

NORM_EPS = 1e-6
MESH = pl.DeviceIdType.MESH
F32 = jnp.float32
BF16 = jnp.bfloat16

OWN0, OPP0, OPP1, RIGHT0, LEFT0, RIGHT1, LEFT1, OWN1 = range(8)
UNITS = 8
CHUNK = 256
LAYERS = 2


def rms_norm(hidden, gain):
    inv_rms = lax.rsqrt(jnp.mean(hidden * hidden, axis=-1, keepdims=True) + NORM_EPS)
    return (hidden * inv_rms * gain).astype(BF16)


def body(
    ep_size, heads, kv_heads, top_k, rows_half,
    x_ref, *refs,
):
    layer_refs = (refs[:12], refs[12:24])
    (
        out_ref,
        wqkv, wo, ub, mb, ms, wg, wu, wd, sg, su, sd, acc, xb, hb, keep, dsend, drecv, isend, rbuf,
        asem, wsem, shsem, fs, fr, uss, urs, mss, mrs, dss, drs, iss, irs, credit,
    ) = refs[24:]
    chips = ep_size // 2
    me = lax.axis_index('ep')
    chip, core = me // 2, me % 2
    other = 1 - core
    sib = 2 * chip + other
    left = 2 * ((chip + chips - 1) % chips) + core
    right = 2 * ((chip + 1) % chips) + core
    ff = wg.shape[2]
    model_dim = wg.shape[1]
    half_len = ub.shape[2]
    head_dim = model_dim // heads
    group = heads // kv_heads
    n_ff, n_out = ff // CHUNK, model_dim // CHUNK

    def remote(src, dst, send, recv, device):
        return pltpu.make_async_remote_copy(src_ref=src, dst_ref=dst, send_sem=send, recv_sem=recv, device_id={'ep': device}, device_id_type=MESH)

    def attention_weights(layer):
        wqkv_ref, wo_ref = layer_refs[layer][1:3]
        return (
            pltpu.make_async_copy(wqkv_ref, wqkv, asem.at[0]),
            pltpu.make_async_copy(wo_ref, wo, asem.at[1]),
        )

    def shared_piece(layer, j, slot):
        sg_ref, su_ref, sd_ref = layer_refs[layer][9:12]
        cols = pl.ds(pl.multiple_of(j * CHUNK, CHUNK), CHUNK)
        return (
            pltpu.make_async_copy(sg_ref.at[:, cols], sg.at[slot], shsem.at[slot, 0]),
            pltpu.make_async_copy(su_ref.at[:, cols], su.at[slot], shsem.at[slot, 1]),
            pltpu.make_async_copy(sd_ref.at[cols, :], sd.at[slot], shsem.at[slot, 2]),
        )

    def expert_weights(layer, e):
        wg_ref, wu_ref, wd_ref = layer_refs[layer][6:9]
        return (
            pltpu.make_async_copy(wg_ref.at[e], wg.at[e], wsem.at[e, 0]),
            pltpu.make_async_copy(wu_ref.at[e], wu.at[e], wsem.at[e, 1]),
            pltpu.make_async_copy(wd_ref.at[e], wd.at[e], wsem.at[e, 2]),
        )

    def start_for(layer, make):
        for which in range(LAYERS):
            @pl.when(layer == which)
            def _():
                for copy in make(which):
                    copy.start()

    x_copy = pltpu.make_async_copy(x_ref, out_ref, asem.at[2])
    x_copy.start()
    for copy in attention_weights(0):
        copy.start()

    barrier = pltpu.get_barrier_semaphore()
    for step in range(1, ep_size):
        pl.semaphore_signal(barrier, inc=1, device_id={'ep': (me + step) % ep_size}, device_id_type=MESH)
    x_copy.wait()
    pl.semaphore_wait(barrier, ep_size - 1)

    def ring_u(src, slot, device):
        return remote(src, ub.at[slot, core], uss.at[slot], urs.at[slot], device)

    def arrived(slot):
        ring_u(ub.at[slot, core], slot, left).wait_recv()

    def partner_u(slot):
        return remote(ub.at[slot, core], ub.at[slot, core], fs.at[slot], fr.at[slot], sib)

    def partner_in(slot):
        return remote(ub.at[slot, other], ub.at[slot, other], fs.at[slot], fr.at[slot], sib)

    hops = ((0, (OWN0, OWN1)), (1, (LEFT0, LEFT1)), (2, (OPP0, OPP1)), (3, (RIGHT0, RIGHT1)))

    def meta_sends(h):
        copies = []
        for hop, slots in hops:
            for flip in range(2):
                if hop == 0 and flip == 0:
                    continue
                dest = 2 * ((chip + hop) % chips) + (core + flip) % 2
                slot = slots[h]
                copies.append(remote(ms.at[h, dest], mb.at[slot, core], mss.at[slot, flip], mrs.at[slot, core], dest))
        return copies

    def partial_copy(slot):
        return remote(dsend.at[slot], drecv.at[slot], dss.at[slot], drs.at[slot], sib)

    def ring_copy(n):
        device = 2 * ((chip + 1 + (chips - 2) * ((n + 1) % 2)) % chips) + core
        return remote(isend.at[(n - 1) % 4], rbuf.at[n - 1], iss.at[n], irs.at[n], device)

    def finish(h):
        for n in (RIGHT0 + 2 * h, LEFT0 + 2 * h):
            ring_copy(n).wait_recv()
        out_ref[h] = (acc[h] + rbuf[RIGHT0 - 1 + 2 * h] + rbuf[LEFT0 - 1 + 2 * h]).astype(BF16)

    def per_layer(layer, index):
        return jnp.where(layer == 0, layer_refs[0][index][...].astype(F32), layer_refs[1][index][...].astype(F32))

    def attention_half(layer, h):
        normed = rms_norm(out_ref[h].astype(F32), per_layer(layer, 0))
        for j in range(wqkv.shape[1] // CHUNK):
            cols = slice(j * CHUNK, (j + 1) * CHUNK)
            hb[0:half_len, cols] = jnp.dot(normed, wqkv[:, cols], preferred_element_type=F32).astype(BF16)
        causal = lax.broadcasted_iota(jnp.int32, (half_len, half_len), 0) >= lax.broadcasted_iota(jnp.int32, (half_len, half_len), 1)
        for head in range(heads):
            kv = head // group
            query = hb[0:half_len, head * head_dim:(head + 1) * head_dim]
            keys = hb[0:half_len, (heads + kv) * head_dim:(heads + kv + 1) * head_dim]
            values = hb[0:half_len, (heads + kv_heads + kv) * head_dim:(heads + kv_heads + kv + 1) * head_dim]
            scores = lax.dot_general(query, keys, (((1,), (1,)), ((), ())), preferred_element_type=F32) * (head_dim ** -0.5)
            scores = jnp.where(causal, scores, -1e30)
            weights = jnp.exp(scores - jnp.max(scores, axis=-1, keepdims=True))
            probs = (weights / jnp.sum(weights, axis=-1, keepdims=True)).astype(BF16)
            xb[0, 0:half_len, head * head_dim:(head + 1) * head_dim] = jnp.dot(probs, values, preferred_element_type=F32).astype(BF16)
        for j in range(n_out):
            cols = slice(j * CHUNK, (j + 1) * CHUNK)
            projected = jnp.dot(xb[0, 0:half_len, :], wo[:, cols], preferred_element_type=F32)
            acc[h, :, cols] = (out_ref[h, :, cols].astype(F32) + projected).astype(BF16).astype(F32)
        ub[OWN1 * h, core] = rms_norm(acc[h], per_layer(layer, 3))

    def routing_half(layer, h):
        rows = ub[OWN1 * h, core]
        router = per_layer(layer, 4).astype(BF16)
        num_experts = router.shape[0]
        logits = lax.dot_general(router, rows, (((1,), (1,)), ((), ())), preferred_element_type=F32)
        picked = jnp.where(layer == 0, layer_refs[0][5][h], layer_refs[1][5][h])
        experts = lax.broadcasted_iota(jnp.int32, (num_experts, half_len), 0)
        chosen = picked[0:1, :] == experts
        for j in range(1, top_k):
            chosen = jnp.logical_or(chosen, picked[j:j + 1, :] == experts)
        masked = jnp.where(chosen, logits, -jnp.inf)
        weights = jnp.exp(masked - jnp.max(masked, axis=0, keepdims=True))
        gates = weights / jnp.sum(weights, axis=0, keepdims=True)
        before = (lax.broadcasted_iota(jnp.int32, (half_len, half_len), 0) < lax.broadcasted_iota(jnp.int32, (half_len, half_len), 1)).astype(BF16)
        place = jnp.dot(chosen.astype(F32).astype(BF16), before, preferred_element_type=F32)
        place = jnp.where(chosen, place, -1.0)
        for dest in range(ep_size):
            ms[h, dest, 0:2, :] = gates[2 * dest:2 * dest + 2, :]
            ms[h, dest, 2:4, :] = place[2 * dest:2 * dest + 2, :]
            ms[h, dest, 4:8, :] = jnp.zeros((4, half_len), F32)
        mb[OWN1 * h, core] = ms[h, me]

    def shared_expert(layer):
        def shared_step(j, carry):
            slot = j % 2

            @pl.when(j + 1 < n_ff)
            def _():
                start_for(layer, lambda which: shared_piece(which, j + 1, (j + 1) % 2))

            @pl.when(j == n_ff // 2)
            def _():
                arrived(RIGHT1)
                ring_u(ub.at[RIGHT1, core], OPP1, left).start()
                ring_u(ub.at[OWN0, core], RIGHT0, left).start()
                partner_u(RIGHT1).start()

            for copy in shared_piece(0, j, slot):
                copy.wait()
            for h, own in ((0, OWN0), (1, OWN1)):
                rows = ub[own, core]
                gate_act = jnp.dot(rows, sg[slot], preferred_element_type=F32)
                up_act = jnp.dot(rows, su[slot], preferred_element_type=F32)
                act = (jax.nn.silu(gate_act) * up_act).astype(BF16)
                acc[h] += jnp.dot(act, sd[slot], preferred_element_type=F32)
            return carry

        lax.fori_loop(0, n_ff, shared_step, 0)

    def merge(layer, n):
        slot = n % 2
        partial_copy(slot).wait_recv()

        @pl.when(jnp.logical_or(n == OWN0, n == OWN1))
        def _():
            acc[n // OWN1] += keep[slot] + drecv[slot]

        @pl.when(jnp.logical_and(n > 4, n < OWN1))
        def _():
            ring_copy(n - 4).wait_send()

        for low, high, add in ((OPP0, OPP1, None), (RIGHT0, RIGHT0, OPP0), (LEFT0, RIGHT1, None), (LEFT1, LEFT1, OPP1)):
            @pl.when(jnp.logical_and(n >= low, n <= high))
            def _():
                total = keep[slot] + drecv[slot]
                if add is not None:
                    ring_copy(add).wait_recv()
                    total = total + rbuf[add - 1]
                isend[(n - 1) % 4] = total

        @pl.when(UNITS * layer + n + 2 < UNITS * LAYERS)
        def _():
            pl.semaphore_signal(credit.at[slot], inc=1, device_id={'ep': sib}, device_id_type=MESH)

        @pl.when(jnp.logical_and(n != OWN0, n != OWN1))
        def _():
            ring_copy(n).start()

    def unit_step(layer, n):
        @pl.when(n == OPP0)
        def _():
            shared_expert(layer)
            arrived(OPP0)
            partner_u(OPP0).start()

        partner_in(n).wait_recv()
        for part, kk in ((0, other), (1, core)):
            @pl.when(jnp.logical_or(jnp.logical_and(n != OWN0, n != OWN1), kk != core))
            def _():
                remote(mb.at[n, kk], mb.at[n, kk], mss.at[n, 0], mrs.at[n, kk], sib).wait_recv()

        for part, kk in ((0, other), (1, core)):
            rows = ub[n, kk]
            for e in range(2):
                place = mb[n, kk, 2 + e:3 + e, :].astype(jnp.int32)
                pick = (place == lax.broadcasted_iota(jnp.int32, (rows_half, half_len), 0)).astype(BF16)
                xb[e, part * rows_half:(part + 1) * rows_half, :] = jnp.dot(pick, rows, preferred_element_type=F32).astype(BF16)

        def expert_step(e, carry):
            @pl.when(n == OWN0)
            def _():
                for copy in expert_weights(0, e):
                    copy.wait()

            @pl.when(jnp.logical_and(n == OPP0, e == 1))
            def _():
                arrived(OPP1)
                partner_u(OPP1).start()

            @pl.when(jnp.logical_and(n == OPP1, e == 1))
            def _():
                for slot in (LEFT1, RIGHT0):
                    arrived(slot)
                    partner_u(slot).start()

            rows = xb[e]
            for j in range(n_ff):
                cols = slice(j * CHUNK, (j + 1) * CHUNK)
                gate_act = jnp.dot(rows, wg[e, :, cols], preferred_element_type=F32)
                up_act = jnp.dot(rows, wu[e, :, cols], preferred_element_type=F32)
                hb[:, cols] = (jax.nn.silu(gate_act) * up_act).astype(BF16)

            @pl.when(jnp.logical_and(n == OWN0, e == 1))
            def _():
                arrived(LEFT0)
                ring_u(ub.at[LEFT0, core], OPP0, right).start()
                ring_u(ub.at[OWN1, core], LEFT1, right).start()
                partner_u(LEFT0).start()

            @pl.when(jnp.logical_and(n == LEFT0, e == 0))
            def _():
                for slot in range(UNITS):
                    partner_u(slot).wait_send()
                for slot in range(OPP0, OWN1):
                    ring_u(ub.at[slot, core], slot, right).wait_send()
                for h in range(2):
                    for copy in meta_sends(h):
                        copy.wait_send()

            @pl.when(jnp.logical_and(n > 0, e == 0))
            def _():
                merge(layer, n - 1)

            for j in range(n_out):
                cols = slice(j * CHUNK, (j + 1) * CHUNK)
                xb[e, :, cols] = jnp.dot(hb[...], wd[e, :, cols], preferred_element_type=F32).astype(BF16)
            return carry

        lax.fori_loop(0, 2, expert_step, 0)

        slot = n % 2

        @pl.when(UNITS * layer + n >= 2)
        def _():
            partial_copy(slot).wait_send()
            pl.semaphore_wait(credit.at[slot], 1)

        for part, kk in ((0, other), (1, core)):
            columns = jnp.transpose(mb[n, kk])
            picks = []
            for e in range(2):
                place = columns[:, 2 + e:3 + e].astype(jnp.int32)
                picks.append((place == lax.broadcasted_iota(jnp.int32, (half_len, rows_half), 1)).astype(BF16))
            target = dsend if part == 0 else keep
            for j in range(n_out):
                cols = slice(j * CHUNK, (j + 1) * CHUNK)
                total = None
                for e in range(2):
                    row = jnp.dot(picks[e], xb[e, part * rows_half:(part + 1) * rows_half, cols], preferred_element_type=F32)
                    term = columns[:, e:e + 1] * row
                    total = term if total is None else total + term
                target[slot, :, cols] = total
        partial_copy(slot).start()

    def layer_step(layer, carry):
        start_for(layer, lambda which: shared_piece(which, 0, 0))
        for e in range(2):
            start_for(layer, lambda which: expert_weights(which, e))

        def half_step(h, carry):
            @pl.when(layer > 0)
            def _():
                finish(h)

            @pl.when(h == 0)
            def _():
                for copy in attention_weights(0):
                    copy.wait()

            attention_half(layer, h)
            routing_half(layer, h)

            @pl.when(h == 0)
            def _():
                ring_u(ub.at[OWN0, core], LEFT0, right).start()
                partner_u(OWN0).start()
                for copy in meta_sends(0):
                    copy.start()

            @pl.when(h == 1)
            def _():
                ring_u(ub.at[OWN1, core], RIGHT1, left).start()
                partner_u(OWN1).start()
                for copy in meta_sends(1):
                    copy.start()
            return carry

        lax.fori_loop(0, 2, half_step, 0)

        @pl.when(layer + 1 < LAYERS)
        def _():
            for copy in attention_weights(1):
                copy.start()

        @pl.when(layer > 0)
        def _():
            for n in (RIGHT0, LEFT0, RIGHT1, LEFT1):
                ring_copy(n).wait_send()

        def step(n, carry):
            unit_step(layer, n)
            return carry

        lax.fori_loop(0, UNITS, step, 0)
        merge(layer, OWN1)
        return carry

    lax.fori_loop(0, LAYERS, layer_step, 0)
    for h in range(2):
        finish(h)
    for n in (RIGHT0, LEFT0, RIGHT1, LEFT1):
        ring_copy(n).wait_send()
    for slot in range(2):
        partial_copy(slot).wait_send()


def two_layers(tokens, layers, ep_size):
    halves, half_len, model_dim = tokens.shape
    operands = [tokens]
    anyspec = pl.BlockSpec(memory_space=pl.ANY)
    vmem = pl.BlockSpec(memory_space=pltpu.VMEM)
    specs = [anyspec]
    for params in layers:
        (attn_gain, w_query, w_key, w_value, w_out, moe_gain, w_router, routes, w_gate, w_up, w_down, shared_gate, shared_up, shared_down) = params
        heads, kv_heads = w_query.shape[1], w_key.shape[1]
        w_qkv = jnp.concatenate([w.reshape(model_dim, -1) for w in (w_query, w_key, w_value)], axis=1)
        operands += [
            attn_gain.reshape(1, model_dim), w_qkv, w_out.reshape(-1, model_dim), moe_gain.reshape(1, model_dim), w_router.T, jnp.swapaxes(routes, 1, 2),
            w_gate, w_up, w_down, shared_gate, shared_up, shared_down,
        ]
        specs += [vmem, anyspec, anyspec, vmem, vmem, vmem] + [anyspec] * 6
    ff = w_gate.shape[2]
    top_k = routes.shape[-1]
    num_experts = w_gate.shape[0] * ep_size
    rows_half = 3 * half_len * top_k // num_experts
    block = (half_len, model_dim)
    dma = pltpu.SemaphoreType.DMA
    return pl.pallas_call(
        functools.partial(body, ep_size, heads, kv_heads, top_k, rows_half),
        out_shape=jax.ShapeDtypeStruct(tokens.shape, BF16),
        in_specs=specs,
        out_specs=vmem,
        scratch_shapes=[
            pltpu.VMEM(w_qkv.shape, BF16),
            pltpu.VMEM((heads * w_query.shape[2], model_dim), BF16),
            pltpu.VMEM((UNITS, 2) + block, BF16),
            pltpu.VMEM((UNITS, 2, 8, half_len), F32),
            pltpu.VMEM((2, ep_size, 8, half_len), F32),
            pltpu.VMEM((2, model_dim, ff), BF16),
            pltpu.VMEM((2, model_dim, ff), BF16),
            pltpu.VMEM((2, ff, model_dim), BF16),
            pltpu.VMEM((2, model_dim, CHUNK), BF16),
            pltpu.VMEM((2, model_dim, CHUNK), BF16),
            pltpu.VMEM((2, CHUNK, model_dim), BF16),
            pltpu.VMEM((2,) + block, F32),
            pltpu.VMEM((2, 2 * rows_half, model_dim), BF16),
            pltpu.VMEM((2 * rows_half, ff), BF16),
            pltpu.VMEM((2,) + block, F32),
            pltpu.VMEM((2,) + block, F32),
            pltpu.VMEM((2,) + block, F32),
            pltpu.VMEM((4,) + block, F32),
            pltpu.VMEM((6,) + block, F32),
            dma((3,)), dma((2, 3)), dma((2, 3)),
            dma((UNITS,)), dma((UNITS,)), dma((UNITS,)), dma((UNITS,)),
            dma((UNITS, 2)), dma((UNITS, 2)),
            dma((2,)), dma((2,)), dma((UNITS,)), dma((UNITS,)),
            pltpu.SemaphoreType.REGULAR((2,)),
        ],
        compiler_params=pltpu.CompilerParams(collective_id=0, has_side_effects=True, vmem_limit_bytes=67043328),
        name='two_layers',
    )(*operands)


def solution(mesh):
    ep_size = mesh.shape['ep']
    token_spec = P(('dp', 'ep'))
    layer_specs = (P(), P(), P(), P(), P(), P(), P(), token_spec, P('ep'), P('ep'), P('ep'), P(), P(), P())
    in_specs = (token_spec,) + layer_specs + layer_specs

    def local_step(tokens, *params):
        return two_layers(tokens, (params[:14], params[14:]), ep_size)

    return jax.shard_map(local_step, mesh=mesh, in_specs=in_specs, out_specs=token_spec, check_vma=False)
```

```python
import functools

import jax
import jax.numpy as jnp
from jax import lax
from jax.experimental import pallas as pl
from jax.experimental.pallas import tpu as pltpu
from jax.sharding import PartitionSpec as P

NORM_EPS = 1e-6
MESH = pl.DeviceIdType.MESH
F32 = jnp.float32
BF16 = jnp.bfloat16

OWN0, LEFT0, OPP0, OPP1, RIGHT0, LEFT1, RIGHT1, OWN1 = range(8)
UNITS = 8
CHUNK = 256
LAYERS = 2


def rms_norm(hidden, gain):
    inv_rms = lax.rsqrt(jnp.mean(hidden * hidden, axis=-1, keepdims=True) + NORM_EPS)
    return (hidden * inv_rms * gain).astype(BF16)


def body(
    ep_size, heads, kv_heads, top_k, rows_half,
    x_ref, *refs,
):
    layer_refs = (refs[:14], refs[14:28])
    (
        out_ref,
        wqkv, wo, ub, mb, ms, wg, wu, wd, sg, su, sd, acc, xb, hb, keep, dsend, drecv, isend, rbuf,
        asem, wsem, shsem, fs, fr, uss, urs, mss, mrs, dss, drs, iss, irs, credit,
    ) = refs[28:]
    chips = ep_size // 2
    me = lax.axis_index('ep')
    chip, core = me // 2, me % 2
    other = 1 - core
    sib = 2 * chip + other
    left = 2 * ((chip + chips - 1) % chips) + core
    right = 2 * ((chip + 1) % chips) + core
    ff = wg.shape[2]
    model_dim = wg.shape[1]
    half_len = ub.shape[2]
    head_dim = model_dim // heads
    group = heads // kv_heads
    n_ff, n_out = ff // CHUNK, model_dim // CHUNK

    def remote(src, dst, send, recv, device):
        return pltpu.make_async_remote_copy(src_ref=src, dst_ref=dst, send_sem=send, recv_sem=recv, device_id={'ep': device}, device_id_type=MESH)

    def attention_weights(layer):
        copies, start = [], 0
        for i, ref in enumerate(layer_refs[layer][1:4]):
            copies.append(pltpu.make_async_copy(ref, wqkv.at[:, pl.ds(start, ref.shape[1])], asem.at[i]))
            start += ref.shape[1]
        copies.append(pltpu.make_async_copy(layer_refs[layer][4], wo, asem.at[3]))
        return copies

    def shared_piece(layer, j, slot):
        sg_ref, su_ref, sd_ref = layer_refs[layer][11:14]
        cols = pl.ds(pl.multiple_of(j * CHUNK, CHUNK), CHUNK)
        return (
            pltpu.make_async_copy(sg_ref.at[:, cols], sg.at[slot], shsem.at[slot, 0]),
            pltpu.make_async_copy(su_ref.at[:, cols], su.at[slot], shsem.at[slot, 1]),
            pltpu.make_async_copy(sd_ref.at[cols, :], sd.at[slot], shsem.at[slot, 2]),
        )

    def expert_weights(layer, e):
        wg_ref, wu_ref, wd_ref = layer_refs[layer][8:11]
        return (
            pltpu.make_async_copy(wg_ref.at[e], wg.at[e], wsem.at[e, 0]),
            pltpu.make_async_copy(wu_ref.at[e], wu.at[e], wsem.at[e, 1]),
            pltpu.make_async_copy(wd_ref.at[e], wd.at[e], wsem.at[e, 2]),
        )

    def start_for(layer, make):
        for which in range(LAYERS):
            @pl.when(layer == which)
            def _():
                for copy in make(which):
                    copy.start()

    x_copy = pltpu.make_async_copy(x_ref, out_ref, asem.at[4])
    x_copy.start()
    for copy in attention_weights(0):
        copy.start()

    barrier = pltpu.get_barrier_semaphore()
    for step in range(1, ep_size):
        pl.semaphore_signal(barrier, inc=1, device_id={'ep': (me + step) % ep_size}, device_id_type=MESH)
    x_copy.wait()
    pl.semaphore_wait(barrier, ep_size - 1)

    def ring_u(src, slot, device):
        return remote(src, ub.at[slot, core], uss.at[slot], urs.at[slot], device)

    def arrived(slot):
        ring_u(ub.at[slot, core], slot, left).wait_recv()

    def partner_u(slot):
        return remote(ub.at[slot, core], ub.at[slot, core], fs.at[slot], fr.at[slot], sib)

    def partner_in(slot):
        return remote(ub.at[slot, other], ub.at[slot, other], fs.at[slot], fr.at[slot], sib)

    hops = ((0, (OWN0, OWN1)), (1, (LEFT0, LEFT1)), (2, (OPP0, OPP1)), (3, (RIGHT0, RIGHT1)))

    def meta_sends(h):
        copies = []
        for hop, slots in hops:
            for flip in range(2):
                if hop == 0 and flip == 0:
                    continue
                dest = 2 * ((chip + hop) % chips) + (core + flip) % 2
                slot = slots[h]
                copies.append(remote(ms.at[h, dest], mb.at[slot, core], mss.at[slot, flip], mrs.at[slot, core], dest))
        return copies

    def partial_copy(slot):
        return remote(dsend.at[slot], drecv.at[slot], dss.at[slot], drs.at[slot], sib)

    def place_of(n):
        return n - 1 - 3 * (n // LEFT1)

    def ring_copy(n):
        device = right if n in (RIGHT0, RIGHT1) else left
        return remote(isend.at[place_of(n)], rbuf.at[n - 1], iss.at[n, 0], irs.at[n, 0], device)

    def opposite_copy(n, part):
        rows = pl.ds(part * (half_len // 2), half_len // 2)
        return remote(isend.at[place_of(n), rows], rbuf.at[n - 1, rows], iss.at[n, part], irs.at[n, part], (right, left)[part])

    def finish(h):
        from_left, from_right = RIGHT0 + (RIGHT1 - RIGHT0) * h, LEFT0 + (LEFT1 - LEFT0) * h
        for n in (from_left, from_right):
            remote(rbuf.at[n - 1], rbuf.at[n - 1], iss.at[n, 0], irs.at[n, 0], sib).wait_recv()
        out_ref[h] = (acc[h] + rbuf[from_left - 1] + rbuf[from_right - 1]).astype(BF16)

    def per_layer(layer, index):
        return jnp.where(layer == 0, layer_refs[0][index][...].astype(F32), layer_refs[1][index][...].astype(F32))

    def gain_of(layer, index):
        return per_layer(layer, index).reshape(1, model_dim)

    def attention_half(layer, h):
        normed = rms_norm(out_ref[h].astype(F32), gain_of(layer, 0))
        for j in range(wqkv.shape[1] // CHUNK):
            cols = slice(j * CHUNK, (j + 1) * CHUNK)
            hb[0:half_len, cols] = jnp.dot(normed, wqkv[:, cols], preferred_element_type=F32).astype(BF16)
        causal = lax.broadcasted_iota(jnp.int32, (half_len, half_len), 0) >= lax.broadcasted_iota(jnp.int32, (half_len, half_len), 1)
        for head in range(heads):
            kv = head // group
            query = hb[0:half_len, head * head_dim:(head + 1) * head_dim]
            keys = hb[0:half_len, (heads + kv) * head_dim:(heads + kv + 1) * head_dim]
            values = hb[0:half_len, (heads + kv_heads + kv) * head_dim:(heads + kv_heads + kv + 1) * head_dim]
            scores = lax.dot_general(query, keys, (((1,), (1,)), ((), ())), preferred_element_type=F32) * (head_dim ** -0.5)
            scores = jnp.where(causal, scores, -1e30)
            weights = jnp.exp(scores - jnp.max(scores, axis=-1, keepdims=True))
            probs = (weights / jnp.sum(weights, axis=-1, keepdims=True)).astype(BF16)
            xb[0, 0:half_len, head * head_dim:(head + 1) * head_dim] = jnp.dot(probs, values, preferred_element_type=F32).astype(BF16)
        for j in range(n_out):
            cols = slice(j * CHUNK, (j + 1) * CHUNK)
            projected = jnp.dot(xb[0, 0:half_len, :], wo[:, cols], preferred_element_type=F32)
            acc[h, :, cols] = (out_ref[h, :, cols].astype(F32) + projected).astype(BF16).astype(F32)
        ub[OWN1 * h, core] = rms_norm(acc[h], gain_of(layer, 5))

    def routing_half(layer, h):
        rows = ub[OWN1 * h, core]
        router = per_layer(layer, 6).astype(BF16)
        num_experts = router.shape[0]
        logits = lax.dot_general(router, rows, (((1,), (1,)), ((), ())), preferred_element_type=F32)
        picked = jnp.where(layer == 0, layer_refs[0][7][h], layer_refs[1][7][h])
        experts = lax.broadcasted_iota(jnp.int32, (num_experts, half_len), 0)
        chosen = picked[0:1, :] == experts
        for j in range(1, top_k):
            chosen = jnp.logical_or(chosen, picked[j:j + 1, :] == experts)
        masked = jnp.where(chosen, logits, -jnp.inf)
        weights = jnp.exp(masked - jnp.max(masked, axis=0, keepdims=True))
        gates = weights / jnp.sum(weights, axis=0, keepdims=True)
        before = (lax.broadcasted_iota(jnp.int32, (half_len, half_len), 0) < lax.broadcasted_iota(jnp.int32, (half_len, half_len), 1)).astype(BF16)
        place = jnp.dot(chosen.astype(F32).astype(BF16), before, preferred_element_type=F32)
        place = jnp.where(chosen, place, -1.0)
        for dest in range(ep_size):
            ms[h, dest, 0:2, :] = gates[2 * dest:2 * dest + 2, :]
            ms[h, dest, 2:4, :] = place[2 * dest:2 * dest + 2, :]
            ms[h, dest, 4:8, :] = jnp.zeros((4, half_len), F32)
        mb[OWN1 * h, core] = ms[h, me]

    def shared_expert(layer):
        def shared_step(j, carry):
            slot = j % 2

            @pl.when(j + 1 < n_ff)
            def _():
                start_for(layer, lambda which: shared_piece(which, j + 1, (j + 1) % 2))

            for copy in shared_piece(0, j, slot):
                copy.wait()
            for h, own in ((0, OWN0), (1, OWN1)):
                rows = ub[own, core]
                gate_act = jnp.dot(rows, sg[slot], preferred_element_type=F32)
                up_act = jnp.dot(rows, su[slot], preferred_element_type=F32)
                act = (jax.nn.silu(gate_act) * up_act).astype(BF16)
                acc[h] += jnp.dot(act, sd[slot], preferred_element_type=F32)
            return carry

        lax.fori_loop(0, n_ff, shared_step, 0)

    def merge(layer, n):
        slot = n % 2
        partial_copy(slot).wait_recv()

        @pl.when(jnp.logical_or(n == OWN0, n == OWN1))
        def _():
            acc[n // OWN1] += keep[slot] + drecv[slot]

        for unit in (OPP0, OPP1, LEFT0):
            @pl.when(n == unit)
            def _():
                isend[place_of(unit)] = keep[slot] + drecv[slot]

        for unit, opp, part in ((RIGHT0, OPP0, 0), (LEFT1, OPP1, 1), (RIGHT1, OPP1, 0)):
            @pl.when(n == unit)
            def _():
                if unit == RIGHT0:
                    opposite_copy(OPP0, 1).wait_recv()
                    rest = slice(half_len // 2, half_len)
                    isend[place_of(LEFT0), rest] += rbuf[OPP0 - 1, rest]
                else:
                    for side in range(2):
                        opposite_copy(unit - LEFT1 + OPP0, side).wait_send()
                through = slice(part * (half_len // 2), (part + 1) * (half_len // 2))
                alone = slice((1 - part) * (half_len // 2), (2 - part) * (half_len // 2))
                isend[place_of(unit), alone] = keep[slot, alone] + drecv[slot, alone]
                if unit == RIGHT0:
                    ring_copy(LEFT0).start()
                opposite_copy(opp, part).wait_recv()
                isend[place_of(unit), through] = keep[slot, through] + drecv[slot, through] + rbuf[opp - 1, through]

        @pl.when(UNITS * layer + n + 2 < UNITS * LAYERS)
        def _():
            pl.semaphore_signal(credit.at[slot], inc=1, device_id={'ep': sib}, device_id_type=MESH)

        for unit in (OPP0, OPP1):
            @pl.when(n == unit)
            def _():
                for side in range(2):
                    opposite_copy(unit, side).start()

        for unit in (RIGHT0, LEFT1, RIGHT1):
            @pl.when(n == unit)
            def _():
                ring_copy(unit).start()

    def unit_step(layer, n):
        @pl.when(n == OPP0)
        def _():
            arrived(OPP0)
            partner_u(OPP0).start()

        partner_in(n).wait_recv()
        for part, kk in ((0, other), (1, core)):
            @pl.when(jnp.logical_or(jnp.logical_and(n != OWN0, n != OWN1), kk != core))
            def _():
                remote(mb.at[n, kk], mb.at[n, kk], mss.at[n, 0], mrs.at[n, kk], sib).wait_recv()

        for part, kk in ((0, other), (1, core)):
            picks = []
            for e in range(2):
                place = mb[n, kk, 2 + e:3 + e, :].astype(jnp.int32)
                picks.append((place == lax.broadcasted_iota(jnp.int32, (rows_half, half_len), 0)).astype(BF16))
            pick = jnp.concatenate(picks, axis=0)
            for j in range(n_out):
                cols = slice(j * CHUNK, (j + 1) * CHUNK)
                both = jnp.dot(pick, ub[n, kk, :, cols], preferred_element_type=F32).astype(BF16)
                for e in range(2):
                    xb[e, part * rows_half:(part + 1) * rows_half, cols] = both[e * rows_half:(e + 1) * rows_half]

        def expert_step(e, carry):
            @pl.when(n == OWN0)
            def _():
                for copy in expert_weights(0, e):
                    copy.wait()

            @pl.when(jnp.logical_and(n == OPP0, e == 1))
            def _():
                arrived(OPP1)
                partner_u(OPP1).start()

            @pl.when(jnp.logical_and(n == OPP1, e == 1))
            def _():
                for slot in (LEFT1, RIGHT0):
                    arrived(slot)
                    partner_u(slot).start()

            rows = xb[e]
            for j in range(n_ff):
                cols = slice(j * CHUNK, (j + 1) * CHUNK)
                gate_act = jnp.dot(rows, wg[e, :, cols], preferred_element_type=F32)
                up_act = jnp.dot(rows, wu[e, :, cols], preferred_element_type=F32)
                hb[:, cols] = (jax.nn.silu(gate_act) * up_act).astype(BF16)

            @pl.when(jnp.logical_and(n == OWN0, e == 1))
            def _():
                arrived(LEFT0)
                ring_u(ub.at[LEFT0, core], OPP0, right).start()
                ring_u(ub.at[OWN1, core], LEFT1, right).start()
                partner_u(LEFT0).start()

            @pl.when(jnp.logical_and(n == LEFT0, e == 0))
            def _():
                arrived(RIGHT1)
                ring_u(ub.at[RIGHT1, core], OPP1, left).start()
                ring_u(ub.at[OWN0, core], RIGHT0, left).start()
                partner_u(RIGHT1).start()

            @pl.when(jnp.logical_and(n == RIGHT0, e == 0))
            def _():
                for slot in range(UNITS):
                    partner_u(slot).wait_send()
                for slot in range(LEFT0, OWN1):
                    ring_u(ub.at[slot, core], slot, right).wait_send()
                for h in range(2):
                    for copy in meta_sends(h):
                        copy.wait_send()

            @pl.when(jnp.logical_and(n > 0, e == 0))
            def _():
                merge(layer, n - 1)

            for j in range(n_out):
                cols = slice(j * CHUNK, (j + 1) * CHUNK)
                xb[e, :, cols] = jnp.dot(hb[...], wd[e, :, cols], preferred_element_type=F32).astype(BF16)
            return carry

        lax.fori_loop(0, 2, expert_step, 0)

        slot = n % 2

        @pl.when(UNITS * layer + n >= 2)
        def _():
            partial_copy(slot).wait_send()
            pl.semaphore_wait(credit.at[slot], 1)

        for part, kk in ((0, other), (1, core)):
            columns = jnp.transpose(mb[n, kk])
            picks = []
            for e in range(2):
                place = columns[:, 2 + e:3 + e].astype(jnp.int32)
                picks.append((place == lax.broadcasted_iota(jnp.int32, (half_len, rows_half), 1)).astype(BF16))
            target = dsend if part == 0 else keep
            for j in range(n_out):
                cols = slice(j * CHUNK, (j + 1) * CHUNK)
                total = None
                for e in range(2):
                    row = jnp.dot(picks[e], xb[e, part * rows_half:(part + 1) * rows_half, cols], preferred_element_type=F32)
                    term = columns[:, e:e + 1] * row
                    total = term if total is None else total + term
                target[slot, :, cols] = total
        partial_copy(slot).start()

    def layer_step(layer, carry):
        for e in range(2):
            start_for(layer, lambda which: expert_weights(which, e))
        start_for(layer, lambda which: shared_piece(which, 0, 0))

        def half_step(h, carry):
            @pl.when(layer > 0)
            def _():
                finish(h)

            @pl.when(h == 0)
            def _():
                for copy in attention_weights(0):
                    copy.wait()

            attention_half(layer, h)
            routing_half(layer, h)

            @pl.when(h == 0)
            def _():
                ring_u(ub.at[OWN0, core], LEFT0, right).start()
                partner_u(OWN0).start()
                for copy in meta_sends(0):
                    copy.start()

            @pl.when(h == 1)
            def _():
                ring_u(ub.at[OWN1, core], RIGHT1, left).start()
                partner_u(OWN1).start()
                for copy in meta_sends(1):
                    copy.start()
            return carry

        lax.fori_loop(0, 2, half_step, 0)

        @pl.when(layer + 1 < LAYERS)
        def _():
            for copy in attention_weights(1):
                copy.start()

        @pl.when(layer > 0)
        def _():
            for n in (RIGHT0, LEFT0, RIGHT1, LEFT1):
                ring_copy(n).wait_send()

        def step(n, carry):
            unit_step(layer, n)
            return carry

        lax.fori_loop(0, UNITS, step, 0)
        shared_expert(layer)
        merge(layer, OWN1)
        return carry

    lax.fori_loop(0, LAYERS, layer_step, 0)
    for h in range(2):
        finish(h)
    for n in (RIGHT0, LEFT0, RIGHT1, LEFT1):
        ring_copy(n).wait_send()
    for slot in range(2):
        partial_copy(slot).wait_send()


def two_layers(tokens, layers, ep_size):
    halves, half_len, model_dim = tokens.shape
    operands = [tokens]
    anyspec = pl.BlockSpec(memory_space=pl.ANY)
    vmem = pl.BlockSpec(memory_space=pltpu.VMEM)
    specs = [anyspec]
    for params in layers:
        (attn_gain, w_query, w_key, w_value, w_out, moe_gain, w_router, routes, w_gate, w_up, w_down, shared_gate, shared_up, shared_down) = params
        heads, kv_heads, head_dim = w_query.shape[1], w_key.shape[1], w_query.shape[2]
        operands += [
            attn_gain, w_query.reshape(model_dim, -1), w_key.reshape(model_dim, -1), w_value.reshape(model_dim, -1), w_out.reshape(-1, model_dim),
            moe_gain, w_router.T, jnp.swapaxes(routes, 1, 2),
            w_gate, w_up, w_down, shared_gate, shared_up, shared_down,
        ]
        specs += [vmem, anyspec, anyspec, anyspec, anyspec, vmem, vmem, vmem] + [anyspec] * 6
    ff = w_gate.shape[2]
    top_k = routes.shape[-1]
    num_experts = w_gate.shape[0] * ep_size
    rows_half = 3 * half_len * top_k // num_experts
    block = (half_len, model_dim)
    dma = pltpu.SemaphoreType.DMA
    return pl.pallas_call(
        functools.partial(body, ep_size, heads, kv_heads, top_k, rows_half),
        out_shape=jax.ShapeDtypeStruct(tokens.shape, BF16),
        in_specs=specs,
        out_specs=vmem,
        scratch_shapes=[
            pltpu.VMEM((model_dim, (heads + 2 * kv_heads) * head_dim), BF16),
            pltpu.VMEM((heads * head_dim, model_dim), BF16),
            pltpu.VMEM((UNITS, 2) + block, BF16),
            pltpu.VMEM((UNITS, 2, 8, half_len), F32),
            pltpu.VMEM((2, ep_size, 8, half_len), F32),
            pltpu.VMEM((2, model_dim, ff), BF16),
            pltpu.VMEM((2, model_dim, ff), BF16),
            pltpu.VMEM((2, ff, model_dim), BF16),
            pltpu.VMEM((2, model_dim, CHUNK), BF16),
            pltpu.VMEM((2, model_dim, CHUNK), BF16),
            pltpu.VMEM((2, CHUNK, model_dim), BF16),
            pltpu.VMEM((2,) + block, F32),
            pltpu.VMEM((2, 2 * rows_half, model_dim), BF16),
            pltpu.VMEM((2 * rows_half, ff), BF16),
            pltpu.VMEM((2,) + block, F32),
            pltpu.VMEM((2,) + block, F32),
            pltpu.VMEM((2,) + block, F32),
            pltpu.VMEM((4,) + block, F32),
            pltpu.VMEM((6,) + block, F32),
            dma((5,)), dma((2, 3)), dma((2, 3)),
            dma((UNITS,)), dma((UNITS,)), dma((UNITS,)), dma((UNITS,)),
            dma((UNITS, 2)), dma((UNITS, 2)),
            dma((2,)), dma((2,)), dma((UNITS, 2)), dma((UNITS, 2)),
            pltpu.SemaphoreType.REGULAR((2,)),
        ],
        compiler_params=pltpu.CompilerParams(collective_id=0, has_side_effects=True, vmem_limit_bytes=67043328),
        name='two_layers',
    )(*operands)


def solution(mesh):
    ep_size = mesh.shape['ep']
    token_spec = P(('dp', 'ep'))
    layer_specs = (P(), P(), P(), P(), P(), P(), P(), token_spec, P('ep'), P('ep'), P('ep'), P(), P(), P())
    in_specs = (token_spec,) + layer_specs + layer_specs

    def local_step(tokens, *params):
        return two_layers(tokens, (params[:14], params[14:]), ep_size)

    return jax.shard_map(local_step, mesh=mesh, in_specs=in_specs, out_specs=token_spec, check_vma=False)
```

```python
import functools

import jax
import jax.numpy as jnp
from jax import lax
from jax.experimental import pallas as pl
from jax.experimental.pallas import tpu as pltpu
from jax.sharding import PartitionSpec as P

NORM_EPS = 1e-6
MESH = pl.DeviceIdType.MESH
F32 = jnp.float32
BF16 = jnp.bfloat16

OWN0, LEFT0, OPP0, OPP1, RIGHT0, LEFT1, RIGHT1, OWN1 = range(8)
UNITS = 8
CHUNK = 256
LAYERS = 2


def rms_norm(hidden, gain):
    inv_rms = lax.rsqrt(jnp.mean(hidden * hidden, axis=-1, keepdims=True) + NORM_EPS)
    return (hidden * inv_rms * gain).astype(BF16)


def body(
    ep_size, heads, kv_heads, top_k, rows_half,
    x_ref, *refs,
):
    layer_refs = (refs[:14], refs[14:28])
    (
        out_ref,
        wqkv, wo, ub, mb, ms, wg, wu, wd, sg, su, sd, acc, xb, hb, keep, dsend, drecv, isend, rbuf,
        asem, wsem, shsem, fs, fr, uss, urs, mss, mrs, dss, drs, iss, irs, credit,
    ) = refs[28:]
    chips = ep_size // 2
    me = lax.axis_index('ep')
    chip, core = me // 2, me % 2
    other = 1 - core
    sib = 2 * chip + other
    left = 2 * ((chip + chips - 1) % chips) + core
    right = 2 * ((chip + 1) % chips) + core
    ff = wg.shape[2]
    model_dim = wg.shape[1]
    half_len = ub.shape[2]
    head_dim = model_dim // heads
    group = heads // kv_heads
    n_ff, n_out = ff // CHUNK, model_dim // CHUNK

    def remote(src, dst, send, recv, device):
        return pltpu.make_async_remote_copy(src_ref=src, dst_ref=dst, send_sem=send, recv_sem=recv, device_id={'ep': device}, device_id_type=MESH)

    def attention_weights(layer):
        copies, start = [], 0
        for i, ref in enumerate(layer_refs[layer][1:4]):
            copies.append(pltpu.make_async_copy(ref, wqkv.at[:, pl.ds(start, ref.shape[1])], asem.at[i]))
            start += ref.shape[1]
        copies.append(pltpu.make_async_copy(layer_refs[layer][4], wo, asem.at[3]))
        return copies

    def shared_piece(layer, j, slot):
        sg_ref, su_ref, sd_ref = layer_refs[layer][11:14]
        cols = pl.ds(pl.multiple_of(j * CHUNK, CHUNK), CHUNK)
        return (
            pltpu.make_async_copy(sg_ref.at[:, cols], sg.at[slot], shsem.at[slot, 0]),
            pltpu.make_async_copy(su_ref.at[:, cols], su.at[slot], shsem.at[slot, 1]),
            pltpu.make_async_copy(sd_ref.at[cols, :], sd.at[slot], shsem.at[slot, 2]),
        )

    def expert_weights(layer, e):
        wg_ref, wu_ref, wd_ref = layer_refs[layer][8:11]
        return (
            pltpu.make_async_copy(wg_ref.at[e], wg.at[e], wsem.at[e, 0]),
            pltpu.make_async_copy(wu_ref.at[e], wu.at[e], wsem.at[e, 1]),
            pltpu.make_async_copy(wd_ref.at[e], wd.at[e], wsem.at[e, 2]),
        )

    def start_for(layer, make):
        for which in range(LAYERS):
            @pl.when(layer == which)
            def _():
                for copy in make(which):
                    copy.start()

    x_copy = pltpu.make_async_copy(x_ref, out_ref, asem.at[4])
    x_copy.start()
    for copy in attention_weights(0):
        copy.start()

    barrier = pltpu.get_barrier_semaphore()
    for step in range(1, ep_size):
        pl.semaphore_signal(barrier, inc=1, device_id={'ep': (me + step) % ep_size}, device_id_type=MESH)
    x_copy.wait()
    pl.semaphore_wait(barrier, ep_size - 1)

    def ring_u(src, slot, part, device):
        rows = pl.ds(part * (half_len // 2), half_len // 2)
        return remote(ub.at[src, core, rows], ub.at[slot, core, rows], uss.at[slot, part], urs.at[slot, part], device)

    def arrived(slot, *parts):
        for part in parts:
            ring_u(slot, slot, part, left).wait_recv()

    def partner_u(slot):
        return remote(ub.at[slot, core], ub.at[slot, core], fs.at[slot], fr.at[slot], sib)

    def partner_in(slot):
        return remote(ub.at[slot, other], ub.at[slot, other], fs.at[slot], fr.at[slot], sib)

    hops = ((0, (OWN0, OWN1)), (1, (LEFT0, LEFT1)), (2, (OPP0, OPP1)), (3, (RIGHT0, RIGHT1)))

    def meta_sends(h):
        copies = []
        for hop, slots in hops:
            for flip in range(2):
                if hop == 0 and flip == 0:
                    continue
                dest = 2 * ((chip + hop) % chips) + (core + flip) % 2
                slot = slots[h]
                copies.append(remote(ms.at[h, dest], mb.at[slot, core], mss.at[slot, flip], mrs.at[slot, core], dest))
        return copies

    def partial_copy(slot):
        return remote(dsend.at[slot], drecv.at[slot], dss.at[slot], drs.at[slot], sib)

    def place_of(n):
        return n - 1 - 3 * (n // LEFT1)

    def ring_copy(n):
        device = right if n in (RIGHT0, RIGHT1) else left
        return remote(isend.at[place_of(n)], rbuf.at[n - 1], iss.at[n, 0], irs.at[n, 0], device)

    def opposite_copy(n, part):
        rows = pl.ds(part * (half_len // 2), half_len // 2)
        return remote(isend.at[place_of(n), rows], rbuf.at[n - 1, rows], iss.at[n, part], irs.at[n, part], (right, left)[part])

    def finish(h):
        from_left, from_right = RIGHT0 + (RIGHT1 - RIGHT0) * h, LEFT0 + (LEFT1 - LEFT0) * h
        for n in (from_left, from_right):
            remote(rbuf.at[n - 1], rbuf.at[n - 1], iss.at[n, 0], irs.at[n, 0], sib).wait_recv()
        out_ref[h] = (acc[h] + rbuf[from_left - 1] + rbuf[from_right - 1]).astype(BF16)

    def per_layer(layer, index):
        return jnp.where(layer == 0, layer_refs[0][index][...].astype(F32), layer_refs[1][index][...].astype(F32))

    def gain_of(layer, index):
        return per_layer(layer, index).reshape(1, model_dim)

    def attention_half(layer, h):
        normed = rms_norm(out_ref[h].astype(F32), gain_of(layer, 0))
        for j in range(wqkv.shape[1] // CHUNK):
            cols = slice(j * CHUNK, (j + 1) * CHUNK)
            hb[0:half_len, cols] = jnp.dot(normed, wqkv[:, cols], preferred_element_type=F32).astype(BF16)
        causal = lax.broadcasted_iota(jnp.int32, (half_len, half_len), 0) >= lax.broadcasted_iota(jnp.int32, (half_len, half_len), 1)
        for head in range(heads):
            kv = head // group
            query = hb[0:half_len, head * head_dim:(head + 1) * head_dim]
            keys = hb[0:half_len, (heads + kv) * head_dim:(heads + kv + 1) * head_dim]
            values = hb[0:half_len, (heads + kv_heads + kv) * head_dim:(heads + kv_heads + kv + 1) * head_dim]
            scores = lax.dot_general(query, keys, (((1,), (1,)), ((), ())), preferred_element_type=F32) * (head_dim ** -0.5)
            scores = jnp.where(causal, scores, -1e30)
            weights = jnp.exp(scores - jnp.max(scores, axis=-1, keepdims=True))
            probs = (weights / jnp.sum(weights, axis=-1, keepdims=True)).astype(BF16)
            xb[0, 0:half_len, head * head_dim:(head + 1) * head_dim] = jnp.dot(probs, values, preferred_element_type=F32).astype(BF16)
        for j in range(n_out):
            cols = slice(j * CHUNK, (j + 1) * CHUNK)
            projected = jnp.dot(xb[0, 0:half_len, :], wo[:, cols], preferred_element_type=F32)
            acc[h, :, cols] = (out_ref[h, :, cols].astype(F32) + projected).astype(BF16).astype(F32)
        ub[OWN1 * h, core] = rms_norm(acc[h], gain_of(layer, 5))

    def routing_half(layer, h):
        rows = ub[OWN1 * h, core]
        router = per_layer(layer, 6).astype(BF16)
        num_experts = router.shape[0]
        logits = lax.dot_general(router, rows, (((1,), (1,)), ((), ())), preferred_element_type=F32)
        picked = jnp.where(layer == 0, layer_refs[0][7][h], layer_refs[1][7][h])
        experts = lax.broadcasted_iota(jnp.int32, (num_experts, half_len), 0)
        chosen = picked[0:1, :] == experts
        for j in range(1, top_k):
            chosen = jnp.logical_or(chosen, picked[j:j + 1, :] == experts)
        masked = jnp.where(chosen, logits, -jnp.inf)
        weights = jnp.exp(masked - jnp.max(masked, axis=0, keepdims=True))
        gates = weights / jnp.sum(weights, axis=0, keepdims=True)
        before = (lax.broadcasted_iota(jnp.int32, (half_len, half_len), 0) < lax.broadcasted_iota(jnp.int32, (half_len, half_len), 1)).astype(BF16)
        place = jnp.dot(chosen.astype(F32).astype(BF16), before, preferred_element_type=F32)
        place = jnp.where(chosen, place, -1.0)
        for dest in range(ep_size):
            ms[h, dest, 0:2, :] = gates[2 * dest:2 * dest + 2, :]
            ms[h, dest, 2:4, :] = place[2 * dest:2 * dest + 2, :]
            ms[h, dest, 4:8, :] = jnp.zeros((4, half_len), F32)
        mb[OWN1 * h, core] = ms[h, me]

    def shared_expert(layer):
        def shared_step(j, carry):
            slot = j % 2

            @pl.when(j + 1 < n_ff)
            def _():
                start_for(layer, lambda which: shared_piece(which, j + 1, (j + 1) % 2))

            for copy in shared_piece(0, j, slot):
                copy.wait()
            for h, own in ((0, OWN0), (1, OWN1)):
                rows = ub[own, core]
                gate_act = jnp.dot(rows, sg[slot], preferred_element_type=F32)
                up_act = jnp.dot(rows, su[slot], preferred_element_type=F32)
                act = (jax.nn.silu(gate_act) * up_act).astype(BF16)
                acc[h] += jnp.dot(act, sd[slot], preferred_element_type=F32)
            return carry

        lax.fori_loop(0, n_ff, shared_step, 0)

    def merge(layer, n):
        slot = n % 2
        partial_copy(slot).wait_recv()

        @pl.when(jnp.logical_or(n == OWN0, n == OWN1))
        def _():
            acc[n // OWN1] += keep[slot] + drecv[slot]

        for unit in (OPP0, OPP1, LEFT0):
            @pl.when(n == unit)
            def _():
                isend[place_of(unit)] = keep[slot] + drecv[slot]

        for unit, opp, part in ((RIGHT0, OPP0, 0), (LEFT1, OPP1, 1), (RIGHT1, OPP1, 0)):
            @pl.when(n == unit)
            def _():
                if unit == RIGHT0:
                    opposite_copy(OPP0, 1).wait_recv()
                    rest = slice(half_len // 2, half_len)
                    isend[place_of(LEFT0), rest] += rbuf[OPP0 - 1, rest]
                else:
                    for side in range(2):
                        opposite_copy(unit - LEFT1 + OPP0, side).wait_send()
                through = slice(part * (half_len // 2), (part + 1) * (half_len // 2))
                alone = slice((1 - part) * (half_len // 2), (2 - part) * (half_len // 2))
                isend[place_of(unit), alone] = keep[slot, alone] + drecv[slot, alone]
                if unit == RIGHT0:
                    ring_copy(LEFT0).start()
                opposite_copy(opp, part).wait_recv()
                isend[place_of(unit), through] = keep[slot, through] + drecv[slot, through] + rbuf[opp - 1, through]

        @pl.when(UNITS * layer + n + 2 < UNITS * LAYERS)
        def _():
            pl.semaphore_signal(credit.at[slot], inc=1, device_id={'ep': sib}, device_id_type=MESH)

        for unit in (OPP0, OPP1):
            @pl.when(n == unit)
            def _():
                for side in range(2):
                    opposite_copy(unit, side).start()

        for unit in (RIGHT0, LEFT1, RIGHT1):
            @pl.when(n == unit)
            def _():
                ring_copy(unit).start()

    def unit_step(layer, n):
        @pl.when(n == OWN0)
        def _():
            for copy in expert_weights(0, 0)[:2]:
                copy.wait()

        partner_in(n).wait_recv()
        for part, kk in ((0, other), (1, core)):
            @pl.when(jnp.logical_or(jnp.logical_and(n != OWN0, n != OWN1), kk != core))
            def _():
                remote(mb.at[n, kk], mb.at[n, kk], mss.at[n, 0], mrs.at[n, kk], sib).wait_recv()

        for part, kk in ((0, other), (1, core)):
            picks = []
            for e in range(2):
                place = mb[n, kk, 2 + e:3 + e, :].astype(jnp.int32)
                picks.append((place == lax.broadcasted_iota(jnp.int32, (rows_half, half_len), 0)).astype(BF16))
            pick = jnp.concatenate(picks, axis=0)
            for j in range(n_out):
                cols = slice(j * CHUNK, (j + 1) * CHUNK)
                both = jnp.dot(pick, ub[n, kk, :, cols], preferred_element_type=F32).astype(BF16)
                for e in range(2):
                    xb[e, part * rows_half:(part + 1) * rows_half, cols] = both[e * rows_half:(e + 1) * rows_half]

        def up(e):
            rows = xb[e]
            for j in range(n_ff):
                cols = slice(j * CHUNK, (j + 1) * CHUNK)
                gate_act = jnp.dot(rows, wg[e, :, cols], preferred_element_type=F32)
                up_act = jnp.dot(rows, wu[e, :, cols], preferred_element_type=F32)
                hb[:, cols] = (jax.nn.silu(gate_act) * up_act).astype(BF16)

        def down(e):
            for j in range(n_out):
                cols = slice(j * CHUNK, (j + 1) * CHUNK)
                xb[e, :, cols] = jnp.dot(hb[...], wd[e, :, cols], preferred_element_type=F32).astype(BF16)

        up(0)

        @pl.when(n == OWN0)
        def _():
            arrived(LEFT0, 0)
            ring_u(LEFT0, OPP0, 0, right).start()
            ring_u(OWN1, LEFT1, 0, right).start()
            arrived(RIGHT0, 1)
            ring_u(RIGHT0, OPP0, 1, left).start()
            for copy in expert_weights(0, 0)[2:] + expert_weights(0, 1):
                copy.wait()

        @pl.when(n == LEFT0)
        def _():
            arrived(OPP0, 0, 1)
            partner_u(OPP0).start()

        @pl.when(n == OPP1)
        def _():
            arrived(LEFT1, 1)
            arrived(RIGHT0, 0)
            arrived(RIGHT1, 0)
            for slot in (RIGHT0, LEFT1, RIGHT1):
                partner_u(slot).start()

        @pl.when(n == RIGHT0)
        def _():
            for slot in range(UNITS):
                partner_u(slot).wait_send()
            for slot in range(LEFT0, OWN1):
                for part in range(2):
                    ring_u(slot, slot, part, right).wait_send()
            for h in range(2):
                for copy in meta_sends(h):
                    copy.wait_send()

        @pl.when(n > 0)
        def _():
            merge(layer, n - 1)

        down(0)
        up(1)

        @pl.when(n == OWN0)
        def _():
            arrived(LEFT0, 1)
            partner_u(LEFT0).start()
            arrived(RIGHT1, 1)
            ring_u(RIGHT1, OPP1, 1, left).start()
            ring_u(OWN0, RIGHT0, 0, left).start()
            ring_u(OWN1, RIGHT1, 0, left).start()

        @pl.when(n == LEFT0)
        def _():
            arrived(LEFT1, 0)
            ring_u(LEFT1, OPP1, 0, right).start()
            ring_u(OWN1, LEFT1, 1, right).start()

        @pl.when(n == OPP0)
        def _():
            arrived(OPP1, 0, 1)
            partner_u(OPP1).start()

        slot = n % 2

        @pl.when(UNITS * layer + n >= 2)
        def _():
            partial_copy(slot).wait_send()
            pl.semaphore_wait(credit.at[slot], 1)

        down(1)

        for part, kk in ((0, other), (1, core)):
            columns = jnp.transpose(mb[n, kk])
            picks = []
            for e in range(2):
                place = columns[:, 2 + e:3 + e].astype(jnp.int32)
                picks.append((place == lax.broadcasted_iota(jnp.int32, (half_len, rows_half), 1)).astype(BF16))
            target = dsend if part == 0 else keep
            for j in range(n_out):
                cols = slice(j * CHUNK, (j + 1) * CHUNK)
                total = None
                for e in range(2):
                    row = jnp.dot(picks[e], xb[e, part * rows_half:(part + 1) * rows_half, cols], preferred_element_type=F32)
                    term = columns[:, e:e + 1] * row
                    total = term if total is None else total + term
                target[slot, :, cols] = total
        partial_copy(slot).start()

    def layer_step(layer, carry):
        for e in range(2):
            start_for(layer, lambda which: expert_weights(which, e))
        start_for(layer, lambda which: shared_piece(which, 0, 0))

        def half_step(h, carry):
            @pl.when(layer > 0)
            def _():
                finish(h)

            @pl.when(h == 0)
            def _():
                for copy in attention_weights(0):
                    copy.wait()

            attention_half(layer, h)
            routing_half(layer, h)

            @pl.when(h == 0)
            def _():
                ring_u(OWN0, LEFT0, 0, right).start()
                ring_u(OWN0, RIGHT0, 1, left).start()
                ring_u(OWN0, LEFT0, 1, right).start()
                partner_u(OWN0).start()
                for copy in meta_sends(0):
                    copy.start()

            @pl.when(h == 1)
            def _():
                ring_u(OWN1, RIGHT1, 1, left).start()
                partner_u(OWN1).start()
                for copy in meta_sends(1):
                    copy.start()
            return carry

        lax.fori_loop(0, 2, half_step, 0)

        @pl.when(layer + 1 < LAYERS)
        def _():
            for copy in attention_weights(1):
                copy.start()

        @pl.when(layer > 0)
        def _():
            for n in (RIGHT0, LEFT0, RIGHT1, LEFT1):
                ring_copy(n).wait_send()

        def step(n, carry):
            unit_step(layer, n)
            return carry

        lax.fori_loop(0, UNITS, step, 0)
        shared_expert(layer)
        merge(layer, OWN1)
        return carry

    lax.fori_loop(0, LAYERS, layer_step, 0)
    for h in range(2):
        finish(h)
    for n in (RIGHT0, LEFT0, RIGHT1, LEFT1):
        ring_copy(n).wait_send()
    for slot in range(2):
        partial_copy(slot).wait_send()


def two_layers(tokens, layers, ep_size):
    halves, half_len, model_dim = tokens.shape
    operands = [tokens]
    anyspec = pl.BlockSpec(memory_space=pl.ANY)
    vmem = pl.BlockSpec(memory_space=pltpu.VMEM)
    specs = [anyspec]
    for params in layers:
        (attn_gain, w_query, w_key, w_value, w_out, moe_gain, w_router, routes, w_gate, w_up, w_down, shared_gate, shared_up, shared_down) = params
        heads, kv_heads, head_dim = w_query.shape[1], w_key.shape[1], w_query.shape[2]
        operands += [
            attn_gain, w_query.reshape(model_dim, -1), w_key.reshape(model_dim, -1), w_value.reshape(model_dim, -1), w_out.reshape(-1, model_dim),
            moe_gain, w_router.T, jnp.swapaxes(routes, 1, 2),
            w_gate, w_up, w_down, shared_gate, shared_up, shared_down,
        ]
        specs += [vmem, anyspec, anyspec, anyspec, anyspec, vmem, vmem, vmem] + [anyspec] * 6
    ff = w_gate.shape[2]
    top_k = routes.shape[-1]
    num_experts = w_gate.shape[0] * ep_size
    rows_half = 3 * half_len * top_k // num_experts
    block = (half_len, model_dim)
    dma = pltpu.SemaphoreType.DMA
    return pl.pallas_call(
        functools.partial(body, ep_size, heads, kv_heads, top_k, rows_half),
        out_shape=jax.ShapeDtypeStruct(tokens.shape, BF16),
        in_specs=specs,
        out_specs=vmem,
        scratch_shapes=[
            pltpu.VMEM((model_dim, (heads + 2 * kv_heads) * head_dim), BF16),
            pltpu.VMEM((heads * head_dim, model_dim), BF16),
            pltpu.VMEM((UNITS, 2) + block, BF16),
            pltpu.VMEM((UNITS, 2, 8, half_len), F32),
            pltpu.VMEM((2, ep_size, 8, half_len), F32),
            pltpu.VMEM((2, model_dim, ff), BF16),
            pltpu.VMEM((2, model_dim, ff), BF16),
            pltpu.VMEM((2, ff, model_dim), BF16),
            pltpu.VMEM((2, model_dim, CHUNK), BF16),
            pltpu.VMEM((2, model_dim, CHUNK), BF16),
            pltpu.VMEM((2, CHUNK, model_dim), BF16),
            pltpu.VMEM((2,) + block, F32),
            pltpu.VMEM((2, 2 * rows_half, model_dim), BF16),
            pltpu.VMEM((2 * rows_half, ff), BF16),
            pltpu.VMEM((2,) + block, F32),
            pltpu.VMEM((2,) + block, F32),
            pltpu.VMEM((2,) + block, F32),
            pltpu.VMEM((4,) + block, F32),
            pltpu.VMEM((6,) + block, F32),
            dma((5,)), dma((2, 3)), dma((2, 3)),
            dma((UNITS,)), dma((UNITS,)), dma((UNITS, 2)), dma((UNITS, 2)),
            dma((UNITS, 2)), dma((UNITS, 2)),
            dma((2,)), dma((2,)), dma((UNITS, 2)), dma((UNITS, 2)),
            pltpu.SemaphoreType.REGULAR((2,)),
        ],
        compiler_params=pltpu.CompilerParams(collective_id=0, has_side_effects=True, vmem_limit_bytes=67043328),
        name='two_layers',
    )(*operands)


def solution(mesh):
    ep_size = mesh.shape['ep']
    token_spec = P(('dp', 'ep'))
    layer_specs = (P(), P(), P(), P(), P(), P(), P(), token_spec, P('ep'), P('ep'), P('ep'), P(), P(), P())
    in_specs = (token_spec,) + layer_specs + layer_specs

    def local_step(tokens, *params):
        return two_layers(tokens, (params[:14], params[14:]), ep_size)

    return jax.shard_map(local_step, mesh=mesh, in_specs=in_specs, out_specs=token_spec, check_vma=False)
```

```python
import functools

import jax
import jax.numpy as jnp
from jax import lax
from jax.experimental import pallas as pl
from jax.experimental.pallas import tpu as pltpu
from jax.sharding import PartitionSpec as P

NORM_EPS = 1e-6
MESH = pl.DeviceIdType.MESH
F32 = jnp.float32
BF16 = jnp.bfloat16

LEFT0, OPP0, OPP1, RIGHT0, LEFT1, RIGHT1, OWN0, OWN1 = range(8)
UNITS = 8
CHUNK = 256
LAYERS = 2


def rms_norm(hidden, gain):
    inv_rms = lax.rsqrt(jnp.mean(hidden * hidden, axis=-1, keepdims=True) + NORM_EPS)
    return (hidden * inv_rms * gain).astype(BF16)


def body(
    ep_size, heads, kv_heads, top_k, rows_half,
    x_ref, *refs,
):
    layer_refs = (refs[:14], refs[14:28])
    (
        out_ref,
        qs, ks, vs, wqkv, wo, ub, mb, ms, wg, wu, wd, sg, su, sd, acc, xb, hb, keep, dsend, drecv, isend, rbuf,
        asem, wsem, shsem, fs, fr, uss, urs, mss, mrs, dss, drs, iss, irs, credit,
    ) = refs[28:]
    chips = ep_size // 2
    me = lax.axis_index('ep')
    chip, core = me // 2, me % 2
    other = 1 - core
    sib = 2 * chip + other
    left = 2 * ((chip + chips - 1) % chips) + core
    right = 2 * ((chip + 1) % chips) + core
    ff = wg.shape[2]
    model_dim = wg.shape[1]
    half_len = ub.shape[2]
    head_dim = model_dim // heads
    group = heads // kv_heads
    n_ff, n_out = ff // CHUNK, model_dim // CHUNK

    def remote(src, dst, send, recv, device):
        return pltpu.make_async_remote_copy(src_ref=src, dst_ref=dst, send_sem=send, recv_sem=recv, device_id={'ep': device}, device_id_type=MESH)

    def attention_weights(layer):
        return [
            pltpu.make_async_copy(ref, target, asem.at[i])
            for i, (ref, target) in enumerate(zip(layer_refs[layer][1:5], (qs, ks, vs, wo)))
        ]

    def place_weights():
        rows = model_dim // 8

        def place(r, carry):
            at = pl.ds(pl.multiple_of(r * rows, rows), rows)
            start = 0
            for staged in (qs, ks, vs):
                count = staged.shape[1]
                by_head = jnp.swapaxes(staged[at], 0, 1)
                for i in range(count):
                    wqkv[at, start + i * head_dim:start + (i + 1) * head_dim] = by_head[i]
                start += count * head_dim
            return carry

        lax.fori_loop(0, 8, place, 0)

    def shared_piece(layer, j, slot):
        sg_ref, su_ref, sd_ref = layer_refs[layer][11:14]
        cols = pl.ds(pl.multiple_of(j * CHUNK, CHUNK), CHUNK)
        return (
            pltpu.make_async_copy(sg_ref.at[:, cols], sg.at[slot], shsem.at[slot, 0]),
            pltpu.make_async_copy(su_ref.at[:, cols], su.at[slot], shsem.at[slot, 1]),
            pltpu.make_async_copy(sd_ref.at[cols, :], sd.at[slot], shsem.at[slot, 2]),
        )

    def expert_weights(layer, e):
        wg_ref, wu_ref, wd_ref = layer_refs[layer][8:11]
        return (
            pltpu.make_async_copy(wg_ref.at[e], wg.at[e], wsem.at[e, 0]),
            pltpu.make_async_copy(wu_ref.at[e], wu.at[e], wsem.at[e, 1]),
            pltpu.make_async_copy(wd_ref.at[e], wd.at[e], wsem.at[e, 2]),
        )

    def start_for(layer, make):
        for which in range(LAYERS):
            @pl.when(layer == which)
            def _():
                for copy in make(which):
                    copy.start()

    x_copy = pltpu.make_async_copy(x_ref, out_ref, asem.at[4])
    x_copy.start()
    for copy in attention_weights(0):
        copy.start()

    barrier = pltpu.get_barrier_semaphore()
    for step in range(1, ep_size):
        pl.semaphore_signal(barrier, inc=1, device_id={'ep': (me + step) % ep_size}, device_id_type=MESH)
    x_copy.wait()
    pl.semaphore_wait(barrier, ep_size - 1)

    def ring_u(src, slot, part, device):
        rows = pl.ds(part * (half_len // 2), half_len // 2)
        return remote(ub.at[src, core, rows], ub.at[slot, core, rows], uss.at[slot, part], urs.at[slot, part], device)

    def arrived(slot, *parts):
        for part in parts:
            ring_u(slot, slot, part, left).wait_recv()

    def partner_u(slot):
        return remote(ub.at[slot, core], ub.at[slot, core], fs.at[slot], fr.at[slot], sib)

    def partner_in(slot):
        return remote(ub.at[slot, other], ub.at[slot, other], fs.at[slot], fr.at[slot], sib)

    hops = ((0, (OWN0, OWN1)), (1, (LEFT0, LEFT1)), (2, (OPP0, OPP1)), (3, (RIGHT0, RIGHT1)))

    def meta_sends(h):
        copies = []
        for hop, slots in hops:
            for flip in range(2):
                if hop == 0 and flip == 0:
                    continue
                dest = 2 * ((chip + hop) % chips) + (core + flip) % 2
                slot = slots[h]
                copies.append(remote(ms.at[h, dest], mb.at[slot, core], mss.at[slot, flip], mrs.at[slot, core], dest))
        return copies

    def partial_copy(slot):
        return remote(dsend.at[slot], drecv.at[slot], dss.at[slot], drs.at[slot], sib)

    def place_of(n):
        return n - 3 * (n // LEFT1)

    def ring_copy(n):
        device = right if n in (RIGHT0, RIGHT1) else left
        return remote(isend.at[place_of(n)], rbuf.at[n], iss.at[n, 0], irs.at[n, 0], device)

    def opposite_copy(n, part):
        rows = pl.ds(part * (half_len // 2), half_len // 2)
        return remote(isend.at[place_of(n), rows], rbuf.at[n, rows], iss.at[n, part], irs.at[n, part], (right, left)[part])

    def finish(h):
        from_left, from_right = RIGHT0 + (RIGHT1 - RIGHT0) * h, LEFT0 + (LEFT1 - LEFT0) * h
        for n in (from_left, from_right):
            remote(rbuf.at[n], rbuf.at[n], iss.at[n, 0], irs.at[n, 0], sib).wait_recv()
        out_ref[h] = (acc[h] + rbuf[from_left] + rbuf[from_right]).astype(BF16)

    def per_layer(layer, index):
        return jnp.where(layer == 0, layer_refs[0][index][...].astype(F32), layer_refs[1][index][...].astype(F32))

    def gain_of(layer, index):
        return per_layer(layer, index).reshape(1, model_dim)

    def attention_half(layer, h):
        normed = rms_norm(out_ref[h].astype(F32), gain_of(layer, 0))
        for j in range(wqkv.shape[1] // CHUNK):
            cols = slice(j * CHUNK, (j + 1) * CHUNK)
            hb[0:half_len, cols] = jnp.dot(normed, wqkv[:, cols], preferred_element_type=F32).astype(BF16)
        causal = lax.broadcasted_iota(jnp.int32, (half_len, half_len), 0) >= lax.broadcasted_iota(jnp.int32, (half_len, half_len), 1)
        for head in range(heads):
            kv = head // group
            query = hb[0:half_len, head * head_dim:(head + 1) * head_dim]
            keys = hb[0:half_len, (heads + kv) * head_dim:(heads + kv + 1) * head_dim]
            values = hb[0:half_len, (heads + kv_heads + kv) * head_dim:(heads + kv_heads + kv + 1) * head_dim]
            scores = lax.dot_general(query, keys, (((1,), (1,)), ((), ())), preferred_element_type=F32) * (head_dim ** -0.5)
            scores = jnp.where(causal, scores, -1e30)
            weights = jnp.exp(scores - jnp.max(scores, axis=-1, keepdims=True))
            probs = (weights / jnp.sum(weights, axis=-1, keepdims=True)).astype(BF16)
            xb[0, 0:half_len, head * head_dim:(head + 1) * head_dim] = jnp.dot(probs, values, preferred_element_type=F32).astype(BF16)
        for j in range(n_out):
            cols = slice(j * CHUNK, (j + 1) * CHUNK)
            projected = jnp.dot(xb[0, 0:half_len, :], wo[:, cols], preferred_element_type=F32)
            acc[h, :, cols] = (out_ref[h, :, cols].astype(F32) + projected).astype(BF16).astype(F32)
        ub[OWN0 + h, core] = rms_norm(acc[h], gain_of(layer, 5))

    def routing_half(layer, h):
        rows = ub[OWN0 + h, core]
        router = per_layer(layer, 6).astype(BF16)
        num_experts = router.shape[0]
        logits = lax.dot_general(router, rows, (((1,), (1,)), ((), ())), preferred_element_type=F32)
        picked = jnp.where(layer == 0, layer_refs[0][7][h], layer_refs[1][7][h])
        experts = lax.broadcasted_iota(jnp.int32, (num_experts, half_len), 0)
        chosen = picked[0:1, :] == experts
        for j in range(1, top_k):
            chosen = jnp.logical_or(chosen, picked[j:j + 1, :] == experts)
        masked = jnp.where(chosen, logits, -jnp.inf)
        weights = jnp.exp(masked - jnp.max(masked, axis=0, keepdims=True))
        gates = weights / jnp.sum(weights, axis=0, keepdims=True)
        before = (lax.broadcasted_iota(jnp.int32, (half_len, half_len), 0) < lax.broadcasted_iota(jnp.int32, (half_len, half_len), 1)).astype(BF16)
        place = jnp.dot(chosen.astype(F32).astype(BF16), before, preferred_element_type=F32)
        place = jnp.where(chosen, place, -1.0)
        for dest in range(ep_size):
            ms[h, dest, 0:2, :] = gates[2 * dest:2 * dest + 2, :]
            ms[h, dest, 2:4, :] = place[2 * dest:2 * dest + 2, :]
            ms[h, dest, 4:8, :] = jnp.zeros((4, half_len), F32)
        mb[OWN0 + h, core] = ms[h, me]

    def shared_expert(layer):
        def shared_step(j, carry):
            slot = j % 2

            @pl.when(j + 1 < n_ff)
            def _():
                start_for(layer, lambda which: shared_piece(which, j + 1, (j + 1) % 2))

            @pl.when(j == n_ff // 2 + 1)
            def _():
                arrived(LEFT0, 0)
                ring_u(LEFT0, OPP0, 0, right).start()
                ring_u(OWN1, LEFT1, 0, right).start()
                arrived(RIGHT0, 1)
                ring_u(RIGHT0, OPP0, 1, left).start()

            for copy in shared_piece(0, j, slot):
                copy.wait()
            for h, own in ((0, OWN0), (1, OWN1)):
                rows = ub[own, core]
                gate_act = jnp.dot(rows, sg[slot], preferred_element_type=F32)
                up_act = jnp.dot(rows, su[slot], preferred_element_type=F32)
                act = (jax.nn.silu(gate_act) * up_act).astype(BF16)
                acc[h] += jnp.dot(act, sd[slot], preferred_element_type=F32)
            return carry

        lax.fori_loop(0, n_ff, shared_step, 0)
        arrived(LEFT0, 1)
        partner_u(LEFT0).start()
        arrived(RIGHT1, 1)
        ring_u(RIGHT1, OPP1, 1, left).start()
        ring_u(OWN0, RIGHT0, 0, left).start()
        ring_u(OWN1, RIGHT1, 0, left).start()

    def merge(layer, n):
        slot = 0
        partial_copy(slot).wait_recv()

        @pl.when(jnp.logical_or(n == OWN0, n == OWN1))
        def _():
            acc[n % 2] += keep[slot] + drecv[slot]

        for unit in (OPP0, OPP1, LEFT0):
            @pl.when(n == unit)
            def _():
                isend[place_of(unit)] = keep[slot] + drecv[slot]

        for unit, opp, part in ((RIGHT0, OPP0, 0), (LEFT1, OPP1, 1), (RIGHT1, OPP1, 0)):
            @pl.when(n == unit)
            def _():
                if unit == RIGHT0:
                    opposite_copy(OPP0, 1).wait_recv()
                    rest = slice(half_len // 2, half_len)
                    isend[place_of(LEFT0), rest] += rbuf[OPP0, rest]
                else:
                    for side in range(2):
                        opposite_copy(unit - LEFT1 + OPP0, side).wait_send()
                through = slice(part * (half_len // 2), (part + 1) * (half_len // 2))
                alone = slice((1 - part) * (half_len // 2), (2 - part) * (half_len // 2))
                isend[place_of(unit), alone] = keep[slot, alone] + drecv[slot, alone]
                if unit == RIGHT0:
                    ring_copy(LEFT0).start()
                opposite_copy(opp, part).wait_recv()
                isend[place_of(unit), through] = keep[slot, through] + drecv[slot, through] + rbuf[opp, through]

        @pl.when(UNITS * layer + n + 1 < UNITS * LAYERS)
        def _():
            pl.semaphore_signal(credit.at[slot], inc=1, device_id={'ep': sib}, device_id_type=MESH)

        for unit in (OPP0, OPP1):
            @pl.when(n == unit)
            def _():
                for side in range(2):
                    opposite_copy(unit, side).start()

        for unit in (RIGHT0, LEFT1, RIGHT1):
            @pl.when(n == unit)
            def _():
                ring_copy(unit).start()

    def unit_step(layer, n):
        @pl.when(n == LEFT0)
        def _():
            for copy in expert_weights(0, 0)[:2]:
                copy.wait()

        @pl.when(n == OPP0)
        def _():
            arrived(LEFT1, 0)
            ring_u(LEFT1, OPP1, 0, right).start()
            ring_u(OWN1, LEFT1, 1, right).start()

        partner_in(n).wait_recv()
        for part, kk in ((0, other), (1, core)):
            @pl.when(jnp.logical_or(jnp.logical_and(n != OWN0, n != OWN1), kk != core))
            def _():
                remote(mb.at[n, kk], mb.at[n, kk], mss.at[n, 0], mrs.at[n, kk], sib).wait_recv()

        for part, kk in ((0, other), (1, core)):
            picks = []
            for e in range(2):
                place = mb[n, kk, 2 + e:3 + e, :].astype(jnp.int32)
                picks.append((place == lax.broadcasted_iota(jnp.int32, (rows_half, half_len), 0)).astype(BF16))
            pick = jnp.concatenate(picks, axis=0)
            for j in range(n_out):
                cols = slice(j * CHUNK, (j + 1) * CHUNK)
                both = jnp.dot(pick, ub[n, kk, :, cols], preferred_element_type=F32).astype(BF16)
                for e in range(2):
                    xb[e, part * rows_half:(part + 1) * rows_half, cols] = both[e * rows_half:(e + 1) * rows_half]

        def up(e, pieces):
            rows = xb[e]
            for j in pieces:
                cols = slice(j * CHUNK, (j + 1) * CHUNK)
                gate_act = jnp.dot(rows, wg[e, :, cols], preferred_element_type=F32)
                up_act = jnp.dot(rows, wu[e, :, cols], preferred_element_type=F32)
                hb[:, cols] = (jax.nn.silu(gate_act) * up_act).astype(BF16)

        def down(e):
            for j in range(n_out):
                cols = slice(j * CHUNK, (j + 1) * CHUNK)
                xb[e, :, cols] = jnp.dot(hb[...], wd[e, :, cols], preferred_element_type=F32).astype(BF16)

        up(0, range(n_ff // 2 + 1))

        @pl.when(n == LEFT0)
        def _():
            for copy in expert_weights(0, 0)[2:] + expert_weights(0, 1):
                copy.wait()

        @pl.when(n == OPP1)
        def _():
            arrived(LEFT1, 1)
            arrived(RIGHT0, 0)
            arrived(RIGHT1, 0)
            for slot in (RIGHT0, LEFT1, RIGHT1):
                partner_u(slot).start()

        @pl.when(n == RIGHT0)
        def _():
            for slot in range(UNITS):
                partner_u(slot).wait_send()
            for slot in range(LEFT0, OWN0):
                for part in range(2):
                    ring_u(slot, slot, part, right).wait_send()
            for h in range(2):
                for copy in meta_sends(h):
                    copy.wait_send()

        @pl.when(n > 0)
        def _():
            merge(layer, n - 1)

        up(0, range(n_ff // 2 + 1, n_ff))
        down(0)
        up(1, range(n_ff))

        @pl.when(n == LEFT0)
        def _():
            arrived(OPP0, 0, 1)
            partner_u(OPP0).start()

        @pl.when(n == OPP0)
        def _():
            arrived(OPP1, 0, 1)
            partner_u(OPP1).start()

        slot = 0

        @pl.when(UNITS * layer + n >= 1)
        def _():
            partial_copy(slot).wait_send()
            pl.semaphore_wait(credit.at[slot], 1)

        down(1)

        for part, kk in ((0, other), (1, core)):
            columns = jnp.transpose(mb[n, kk])
            picks = []
            for e in range(2):
                place = columns[:, 2 + e:3 + e].astype(jnp.int32)
                picks.append((place == lax.broadcasted_iota(jnp.int32, (half_len, rows_half), 1)).astype(BF16))
            target = dsend if part == 0 else keep
            for j in range(n_out):
                cols = slice(j * CHUNK, (j + 1) * CHUNK)
                total = None
                for e in range(2):
                    row = jnp.dot(picks[e], xb[e, part * rows_half:(part + 1) * rows_half, cols], preferred_element_type=F32)
                    term = columns[:, e:e + 1] * row
                    total = term if total is None else total + term
                target[slot, :, cols] = total
        partial_copy(slot).start()

    def layer_step(layer, carry):
        start_for(layer, lambda which: shared_piece(which, 0, 0))
        for e in range(2):
            start_for(layer, lambda which: expert_weights(which, e))

        def half_step(h, carry):
            @pl.when(layer > 0)
            def _():
                finish(h)

            @pl.when(h == 0)
            def _():
                for copy in attention_weights(0):
                    copy.wait()
                place_weights()

            attention_half(layer, h)
            routing_half(layer, h)

            @pl.when(h == 0)
            def _():
                ring_u(OWN0, LEFT0, 0, right).start()
                ring_u(OWN0, RIGHT0, 1, left).start()
                ring_u(OWN0, LEFT0, 1, right).start()
                partner_u(OWN0).start()
                for copy in meta_sends(0):
                    copy.start()

            @pl.when(h == 1)
            def _():
                ring_u(OWN1, RIGHT1, 1, left).start()
                partner_u(OWN1).start()
                for copy in meta_sends(1):
                    copy.start()
            return carry

        lax.fori_loop(0, 2, half_step, 0)

        @pl.when(layer + 1 < LAYERS)
        def _():
            for copy in attention_weights(1):
                copy.start()

        @pl.when(layer > 0)
        def _():
            for n in (RIGHT0, LEFT0, RIGHT1, LEFT1):
                ring_copy(n).wait_send()

        def step(n, carry):
            unit_step(layer, n)
            return carry

        shared_expert(layer)
        lax.fori_loop(0, UNITS, step, 0)
        merge(layer, OWN1)
        return carry

    lax.fori_loop(0, LAYERS, layer_step, 0)
    for h in range(2):
        finish(h)
    for n in (RIGHT0, LEFT0, RIGHT1, LEFT1):
        ring_copy(n).wait_send()
    partial_copy(0).wait_send()


def two_layers(tokens, layers, ep_size):
    halves, half_len, model_dim = tokens.shape
    operands = [tokens]
    anyspec = pl.BlockSpec(memory_space=pl.ANY)
    vmem = pl.BlockSpec(memory_space=pltpu.VMEM)
    specs = [anyspec]
    for params in layers:
        (attn_gain, w_query, w_key, w_value, w_out, moe_gain, w_router, routes, w_gate, w_up, w_down, shared_gate, shared_up, shared_down) = params
        heads, kv_heads, head_dim = w_query.shape[1], w_key.shape[1], w_query.shape[2]
        operands += [
            attn_gain, w_query, w_key, w_value, w_out.reshape(-1, model_dim),
            moe_gain, w_router.T, jnp.swapaxes(routes, 1, 2),
            w_gate, w_up, w_down, shared_gate, shared_up, shared_down,
        ]
        specs += [vmem, anyspec, anyspec, anyspec, anyspec, vmem, vmem, vmem] + [anyspec] * 6
    ff = w_gate.shape[2]
    top_k = routes.shape[-1]
    num_experts = w_gate.shape[0] * ep_size
    rows_half = 3 * half_len * top_k // num_experts
    block = (half_len, model_dim)
    dma = pltpu.SemaphoreType.DMA
    return pl.pallas_call(
        functools.partial(body, ep_size, heads, kv_heads, top_k, rows_half),
        out_shape=jax.ShapeDtypeStruct(tokens.shape, BF16),
        in_specs=specs,
        out_specs=vmem,
        scratch_shapes=[
            pltpu.VMEM(w_query.shape, BF16),
            pltpu.VMEM(w_key.shape, BF16),
            pltpu.VMEM(w_value.shape, BF16),
            pltpu.VMEM((model_dim, (heads + 2 * kv_heads) * head_dim), BF16),
            pltpu.VMEM((heads * head_dim, model_dim), BF16),
            pltpu.VMEM((UNITS, 2) + block, BF16),
            pltpu.VMEM((UNITS, 2, 8, half_len), F32),
            pltpu.VMEM((2, ep_size, 8, half_len), F32),
            pltpu.VMEM((2, model_dim, ff), BF16),
            pltpu.VMEM((2, model_dim, ff), BF16),
            pltpu.VMEM((2, ff, model_dim), BF16),
            pltpu.VMEM((2, model_dim, CHUNK), BF16),
            pltpu.VMEM((2, model_dim, CHUNK), BF16),
            pltpu.VMEM((2, CHUNK, model_dim), BF16),
            pltpu.VMEM((2,) + block, F32),
            pltpu.VMEM((2, 2 * rows_half, model_dim), BF16),
            pltpu.VMEM((2 * rows_half, ff), BF16),
            pltpu.VMEM((1,) + block, F32),
            pltpu.VMEM((1,) + block, F32),
            pltpu.VMEM((1,) + block, F32),
            pltpu.VMEM((4,) + block, F32),
            pltpu.VMEM((6,) + block, F32),
            dma((5,)), dma((2, 3)), dma((2, 3)),
            dma((UNITS,)), dma((UNITS,)), dma((UNITS, 2)), dma((UNITS, 2)),
            dma((UNITS, 2)), dma((UNITS, 2)),
            dma((1,)), dma((1,)), dma((UNITS, 2)), dma((UNITS, 2)),
            pltpu.SemaphoreType.REGULAR((1,)),
        ],
        compiler_params=pltpu.CompilerParams(collective_id=0, has_side_effects=True, vmem_limit_bytes=67043328),
        name='two_layers',
    )(*operands)


def solution(mesh):
    ep_size = mesh.shape['ep']
    token_spec = P(('dp', 'ep'))
    layer_specs = (P(), P(), P(), P(), P(), P(), P(), token_spec, P('ep'), P('ep'), P('ep'), P(), P(), P())
    in_specs = (token_spec,) + layer_specs + layer_specs

    def local_step(tokens, *params):
        return two_layers(tokens, (params[:14], params[14:]), ep_size)

    return jax.shard_map(local_step, mesh=mesh, in_specs=in_specs, out_specs=token_spec, check_vma=False)
```

```python
import functools

import jax
import jax.numpy as jnp
from jax import lax
from jax.experimental import pallas as pl
from jax.experimental.pallas import tpu as pltpu
from jax.sharding import PartitionSpec as P

NORM_EPS = 1e-6
MESH = pl.DeviceIdType.MESH
F32 = jnp.float32
BF16 = jnp.bfloat16

LEFT0, OPP0, OPP1, RIGHT0, LEFT1, RIGHT1, OWN0, OWN1 = range(8)
UNITS = 8
CHUNK = 256
LAYERS = 2


def rms_norm(hidden, gain):
    inv_rms = lax.rsqrt(jnp.mean(hidden * hidden, axis=-1, keepdims=True) + NORM_EPS)
    return (hidden * inv_rms * gain).astype(BF16)


def body(
    ep_size, heads, kv_heads, top_k, rows_half,
    x_ref, *refs,
):
    layer_refs = (refs[:14], refs[14:28])
    (
        out_ref,
        qs, ks, vs, wqkv, wo, ub, mb, ms, wg, wu, wd, sg, su, sd, acc, xb, hb, keep, dsend, drecv, isend, rbuf,
        asem, wsem, shsem, fs, fr, uss, urs, mss, mrs, dss, drs, iss, irs, credit,
    ) = refs[28:]
    chips = ep_size // 2
    me = lax.axis_index('ep')
    chip, core = me // 2, me % 2
    other = 1 - core
    sib = 2 * chip + other
    left = 2 * ((chip + chips - 1) % chips) + core
    right = 2 * ((chip + 1) % chips) + core
    ff = wg.shape[2]
    model_dim = wg.shape[1]
    half_len = ub.shape[2]
    head_dim = model_dim // heads
    group = heads // kv_heads
    n_ff, n_out = ff // CHUNK, model_dim // CHUNK

    def remote(src, dst, send, recv, device):
        return pltpu.make_async_remote_copy(src_ref=src, dst_ref=dst, send_sem=send, recv_sem=recv, device_id={'ep': device}, device_id_type=MESH)

    def attention_weights(layer):
        return [
            pltpu.make_async_copy(ref, target, asem.at[i])
            for i, (ref, target) in enumerate(zip(layer_refs[layer][1:5], (qs, ks, vs, wo)))
        ]

    def place_weights():
        rows = model_dim // 8

        def place(r, carry):
            at = pl.ds(pl.multiple_of(r * rows, rows), rows)
            start = 0
            for staged in (qs, ks, vs):
                count = staged.shape[1]
                by_head = jnp.swapaxes(staged[at], 0, 1)
                for i in range(count):
                    wqkv[at, start + i * head_dim:start + (i + 1) * head_dim] = by_head[i]
                start += count * head_dim
            return carry

        lax.fori_loop(0, 8, place, 0)

    def shared_piece(layer, j, slot):
        sg_ref, su_ref, sd_ref = layer_refs[layer][11:14]
        cols = pl.ds(pl.multiple_of(j * CHUNK, CHUNK), CHUNK)
        return (
            pltpu.make_async_copy(sg_ref.at[:, cols], sg.at[slot], shsem.at[slot, 0]),
            pltpu.make_async_copy(su_ref.at[:, cols], su.at[slot], shsem.at[slot, 1]),
            pltpu.make_async_copy(sd_ref.at[cols, :], sd.at[slot], shsem.at[slot, 2]),
        )

    def expert_weights(layer, e):
        wg_ref, wu_ref, wd_ref = layer_refs[layer][8:11]
        return (
            pltpu.make_async_copy(wg_ref.at[e], wg.at[e], wsem.at[e, 0]),
            pltpu.make_async_copy(wu_ref.at[e], wu.at[e], wsem.at[e, 1]),
            pltpu.make_async_copy(wd_ref.at[e], wd.at[e], wsem.at[e, 2]),
        )

    def start_for(layer, make):
        for which in range(LAYERS):
            @pl.when(layer == which)
            def _():
                for copy in make(which):
                    copy.start()

    x_copy = pltpu.make_async_copy(x_ref, out_ref, asem.at[4])
    x_copy.start()
    for copy in attention_weights(0):
        copy.start()

    barrier = pltpu.get_barrier_semaphore()
    for step in range(1, ep_size):
        pl.semaphore_signal(barrier, inc=1, device_id={'ep': (me + step) % ep_size}, device_id_type=MESH)
    x_copy.wait()
    pl.semaphore_wait(barrier, ep_size - 1)

    def ring_u(src, slot, part, device):
        rows = pl.ds(part * (half_len // 2), half_len // 2)
        return remote(ub.at[src, core, rows], ub.at[slot, core, rows], uss.at[slot, part], urs.at[slot, part], device)

    def arrived(slot, *parts):
        for part in parts:
            ring_u(slot, slot, part, left).wait_recv()

    def partner_u(slot):
        return remote(ub.at[slot, core], ub.at[slot, core], fs.at[slot], fr.at[slot], sib)

    def partner_in(slot):
        return remote(ub.at[slot, other], ub.at[slot, other], fs.at[slot], fr.at[slot], sib)

    hops = ((0, (OWN0, OWN1)), (1, (LEFT0, LEFT1)), (2, (OPP0, OPP1)), (3, (RIGHT0, RIGHT1)))

    def meta_sends(h):
        copies = []
        for hop, slots in hops:
            for flip in range(2):
                if hop == 0 and flip == 0:
                    continue
                dest = 2 * ((chip + hop) % chips) + (core + flip) % 2
                slot = slots[h]
                copies.append(remote(ms.at[h, dest], mb.at[slot, core], mss.at[slot, flip], mrs.at[slot, core], dest))
        return copies

    def partial_copy(slot):
        return remote(dsend.at[slot], drecv.at[slot], dss.at[slot], drs.at[slot], sib)

    def place_of(n):
        return n - 3 * (n // LEFT1)

    def ring_copy(n):
        device = right if n in (RIGHT0, RIGHT1) else left
        return remote(isend.at[place_of(n)], rbuf.at[n], iss.at[n, 0], irs.at[n, 0], device)

    def opposite_copy(n, part):
        rows = pl.ds(part * (half_len // 2), half_len // 2)
        return remote(isend.at[place_of(n), rows], rbuf.at[n, rows], iss.at[n, part], irs.at[n, part], (right, left)[part])

    def finish(h):
        from_left, from_right = RIGHT0 + (RIGHT1 - RIGHT0) * h, LEFT0 + (LEFT1 - LEFT0) * h
        for n in (from_left, from_right):
            remote(rbuf.at[n], rbuf.at[n], iss.at[n, 0], irs.at[n, 0], sib).wait_recv()
        out_ref[h] = (acc[h] + rbuf[from_left] + rbuf[from_right]).astype(BF16)

    def per_layer(layer, index):
        return jnp.where(layer == 0, layer_refs[0][index][...].astype(F32), layer_refs[1][index][...].astype(F32))

    def gain_of(layer, index):
        return per_layer(layer, index).reshape(1, model_dim)

    def attention_half(layer, h):
        normed = rms_norm(out_ref[h].astype(F32), gain_of(layer, 0))
        for j in range(wqkv.shape[1] // CHUNK):
            cols = slice(j * CHUNK, (j + 1) * CHUNK)
            hb[0:half_len, cols] = jnp.dot(normed, wqkv[:, cols], preferred_element_type=F32).astype(BF16)
        causal = lax.broadcasted_iota(jnp.int32, (half_len, half_len), 0) >= lax.broadcasted_iota(jnp.int32, (half_len, half_len), 1)
        for head in range(heads):
            kv = head // group
            query = hb[0:half_len, head * head_dim:(head + 1) * head_dim]
            keys = hb[0:half_len, (heads + kv) * head_dim:(heads + kv + 1) * head_dim]
            values = hb[0:half_len, (heads + kv_heads + kv) * head_dim:(heads + kv_heads + kv + 1) * head_dim]
            scores = lax.dot_general(query, keys, (((1,), (1,)), ((), ())), preferred_element_type=F32) * (head_dim ** -0.5)
            scores = jnp.where(causal, scores, -1e30)
            weights = jnp.exp(scores - jnp.max(scores, axis=-1, keepdims=True))
            probs = (weights / jnp.sum(weights, axis=-1, keepdims=True)).astype(BF16)
            xb[0, 0:half_len, head * head_dim:(head + 1) * head_dim] = jnp.dot(probs, values, preferred_element_type=F32).astype(BF16)
        for j in range(n_out):
            cols = slice(j * CHUNK, (j + 1) * CHUNK)
            projected = jnp.dot(xb[0, 0:half_len, :], wo[:, cols], preferred_element_type=F32)
            acc[h, :, cols] = (out_ref[h, :, cols].astype(F32) + projected).astype(BF16).astype(F32)
        ub[OWN0 + h, core] = rms_norm(acc[h], gain_of(layer, 5))

    def routing_half(layer, h):
        rows = ub[OWN0 + h, core]
        router = per_layer(layer, 6).astype(BF16)
        num_experts = router.shape[0]
        logits = lax.dot_general(router, rows, (((1,), (1,)), ((), ())), preferred_element_type=F32)
        picked = jnp.where(layer == 0, layer_refs[0][7][h], layer_refs[1][7][h])
        experts = lax.broadcasted_iota(jnp.int32, (num_experts, half_len), 0)
        chosen = picked[0:1, :] == experts
        for j in range(1, top_k):
            chosen = jnp.logical_or(chosen, picked[j:j + 1, :] == experts)
        masked = jnp.where(chosen, logits, -jnp.inf)
        weights = jnp.exp(masked - jnp.max(masked, axis=0, keepdims=True))
        gates = weights / jnp.sum(weights, axis=0, keepdims=True)
        before = (lax.broadcasted_iota(jnp.int32, (half_len, half_len), 0) < lax.broadcasted_iota(jnp.int32, (half_len, half_len), 1)).astype(BF16)
        place = jnp.dot(chosen.astype(F32).astype(BF16), before, preferred_element_type=F32)
        place = jnp.where(chosen, place, -1.0)
        for dest in range(ep_size):
            ms[h, dest, 0:2, :] = gates[2 * dest:2 * dest + 2, :]
            ms[h, dest, 2:4, :] = place[2 * dest:2 * dest + 2, :]
            ms[h, dest, 4:8, :] = jnp.zeros((4, half_len), F32)
        mb[OWN0 + h, core] = ms[h, me]

    def shared_expert(layer):
        def shared_step(j, carry):
            slot = j % 2

            @pl.when(j + 1 < n_ff)
            def _():
                start_for(layer, lambda which: shared_piece(which, j + 1, (j + 1) % 2))

            @pl.when(j == n_ff // 2 + 1)
            def _():
                arrived(LEFT0, 0)
                ring_u(LEFT0, OPP0, 0, right).start()
                ring_u(OWN1, LEFT1, 0, right).start()
                arrived(RIGHT0, 1)
                ring_u(RIGHT0, OPP0, 1, left).start()

            for copy in shared_piece(0, j, slot):
                copy.wait()
            for h, own in ((0, OWN0), (1, OWN1)):
                rows = ub[own, core]
                gate_act = jnp.dot(rows, sg[slot], preferred_element_type=F32)
                up_act = jnp.dot(rows, su[slot], preferred_element_type=F32)
                act = (jax.nn.silu(gate_act) * up_act).astype(BF16)
                acc[h] += jnp.dot(act, sd[slot], preferred_element_type=F32)
            return carry

        lax.fori_loop(0, n_ff, shared_step, 0)
        arrived(LEFT0, 1)
        partner_u(LEFT0).start()
        arrived(RIGHT1, 1)
        ring_u(RIGHT1, OPP1, 1, left).start()
        ring_u(OWN0, RIGHT0, 0, left).start()
        ring_u(OWN1, RIGHT1, 0, left).start()

    def merge(layer, n):
        slot = 0
        partial_copy(slot).wait_recv()

        @pl.when(jnp.logical_or(n == OWN0, n == OWN1))
        def _():
            acc[n % 2] += keep[slot] + drecv[slot]

        for unit in (OPP0, OPP1, LEFT0):
            @pl.when(n == unit)
            def _():
                isend[place_of(unit)] = keep[slot] + drecv[slot]

        for unit, opp, part in ((RIGHT0, OPP0, 0), (LEFT1, OPP1, 1), (RIGHT1, OPP1, 0)):
            @pl.when(n == unit)
            def _():
                if unit == RIGHT0:
                    opposite_copy(OPP0, 1).wait_recv()
                    rest = slice(half_len // 2, half_len)
                    isend[place_of(LEFT0), rest] += rbuf[OPP0, rest]
                else:
                    for side in range(2):
                        opposite_copy(unit - LEFT1 + OPP0, side).wait_send()
                through = slice(part * (half_len // 2), (part + 1) * (half_len // 2))
                alone = slice((1 - part) * (half_len // 2), (2 - part) * (half_len // 2))
                isend[place_of(unit), alone] = keep[slot, alone] + drecv[slot, alone]
                if unit == RIGHT0:
                    ring_copy(LEFT0).start()
                opposite_copy(opp, part).wait_recv()
                isend[place_of(unit), through] = keep[slot, through] + drecv[slot, through] + rbuf[opp, through]

        @pl.when(UNITS * layer + n + 1 < UNITS * LAYERS)
        def _():
            pl.semaphore_signal(credit.at[slot], inc=1, device_id={'ep': sib}, device_id_type=MESH)

        for unit in (OPP0, OPP1):
            @pl.when(n == unit)
            def _():
                for side in range(2):
                    opposite_copy(unit, side).start()

        for unit in (RIGHT0, LEFT1, RIGHT1):
            @pl.when(n == unit)
            def _():
                ring_copy(unit).start()

    def unit_step(layer, n):
        @pl.when(n == LEFT0)
        def _():
            for copy in expert_weights(0, 0)[:2]:
                copy.wait()

        @pl.when(n == OPP0)
        def _():
            arrived(LEFT1, 0)
            ring_u(LEFT1, OPP1, 0, right).start()
            ring_u(OWN1, LEFT1, 1, right).start()

        partner_in(n).wait_recv()
        for part, kk in ((0, other), (1, core)):
            @pl.when(jnp.logical_or(jnp.logical_and(n != OWN0, n != OWN1), kk != core))
            def _():
                remote(mb.at[n, kk], mb.at[n, kk], mss.at[n, 0], mrs.at[n, kk], sib).wait_recv()

        for part, kk in ((0, other), (1, core)):
            picks = []
            for e in range(2):
                place = mb[n, kk, 2 + e:3 + e, :].astype(jnp.int32)
                picks.append((place == lax.broadcasted_iota(jnp.int32, (rows_half, half_len), 0)).astype(BF16))
            pick = jnp.concatenate(picks, axis=0)
            for j in range(n_out):
                cols = slice(j * CHUNK, (j + 1) * CHUNK)
                both = jnp.dot(pick, ub[n, kk, :, cols], preferred_element_type=F32).astype(BF16)
                for e in range(2):
                    xb[e, part * rows_half:(part + 1) * rows_half, cols] = both[e * rows_half:(e + 1) * rows_half]

        def up(e, pieces):
            rows = xb[e]
            for j in pieces:
                cols = slice(j * CHUNK, (j + 1) * CHUNK)
                gate_act = jnp.dot(rows, wg[e, :, cols], preferred_element_type=F32)
                up_act = jnp.dot(rows, wu[e, :, cols], preferred_element_type=F32)
                hb[:, cols] = (jax.nn.silu(gate_act) * up_act).astype(BF16)

        def down(e):
            for j in range(n_out):
                cols = slice(j * CHUNK, (j + 1) * CHUNK)
                xb[e, :, cols] = jnp.dot(hb[...], wd[e, :, cols], preferred_element_type=F32).astype(BF16)

        up(0, range(n_ff // 2 + 1))

        @pl.when(n == LEFT0)
        def _():
            for copy in expert_weights(0, 0)[2:] + expert_weights(0, 1):
                copy.wait()

        @pl.when(n == OPP1)
        def _():
            arrived(LEFT1, 1)
            arrived(RIGHT0, 0)
            arrived(RIGHT1, 0)
            for slot in (RIGHT0, LEFT1, RIGHT1):
                partner_u(slot).start()

        @pl.when(n == RIGHT0)
        def _():
            for slot in range(UNITS):
                partner_u(slot).wait_send()
            for slot in range(LEFT0, OWN0):
                for part in range(2):
                    ring_u(slot, slot, part, right).wait_send()
            for h in range(2):
                for copy in meta_sends(h):
                    copy.wait_send()

        @pl.when(n > 0)
        def _():
            merge(layer, n - 1)

        up(0, range(n_ff // 2 + 1, n_ff))
        down(0)
        up(1, range(n_ff))

        @pl.when(n == LEFT0)
        def _():
            arrived(OPP0, 0, 1)
            partner_u(OPP0).start()

        @pl.when(n == OPP0)
        def _():
            arrived(OPP1, 0, 1)
            partner_u(OPP1).start()

        slot = 0

        @pl.when(UNITS * layer + n >= 1)
        def _():
            partial_copy(slot).wait_send()
            pl.semaphore_wait(credit.at[slot], 1)

        down(1)

        for part, kk in ((0, other), (1, core)):
            columns = jnp.transpose(mb[n, kk])
            picks = []
            for e in range(2):
                place = columns[:, 2 + e:3 + e].astype(jnp.int32)
                picks.append((place == lax.broadcasted_iota(jnp.int32, (half_len, rows_half), 1)).astype(BF16))
            target = dsend if part == 0 else keep
            for j in range(n_out):
                cols = slice(j * CHUNK, (j + 1) * CHUNK)
                total = None
                for e in range(2):
                    row = jnp.dot(picks[e], xb[e, part * rows_half:(part + 1) * rows_half, cols], preferred_element_type=F32)
                    term = columns[:, e:e + 1] * row
                    total = term if total is None else total + term
                target[slot, :, cols] = total
        partial_copy(slot).start()

    def layer_step(layer, carry):
        start_for(layer, lambda which: shared_piece(which, 0, 0))
        for e in range(2):
            start_for(layer, lambda which: expert_weights(which, e))

        def half_step(h, carry):
            @pl.when(layer > 0)
            def _():
                finish(h)

            @pl.when(h == 0)
            def _():
                *projections, out_weights = attention_weights(0)
                for copy in projections:
                    copy.wait()
                place_weights()
                out_weights.wait()

            attention_half(layer, h)
            routing_half(layer, h)

            @pl.when(h == 0)
            def _():
                ring_u(OWN0, LEFT0, 0, right).start()
                ring_u(OWN0, RIGHT0, 1, left).start()
                ring_u(OWN0, LEFT0, 1, right).start()
                partner_u(OWN0).start()
                for copy in meta_sends(0):
                    copy.start()

            @pl.when(h == 1)
            def _():
                ring_u(OWN1, RIGHT1, 1, left).start()
                partner_u(OWN1).start()
                for copy in meta_sends(1):
                    copy.start()
            return carry

        lax.fori_loop(0, 2, half_step, 0)

        @pl.when(layer + 1 < LAYERS)
        def _():
            for copy in attention_weights(1):
                copy.start()

        @pl.when(layer > 0)
        def _():
            for n in (RIGHT0, LEFT0, RIGHT1, LEFT1):
                ring_copy(n).wait_send()

        def step(n, carry):
            unit_step(layer, n)
            return carry

        shared_expert(layer)
        lax.fori_loop(0, UNITS, step, 0)
        merge(layer, OWN1)
        return carry

    lax.fori_loop(0, LAYERS, layer_step, 0)
    for h in range(2):
        finish(h)
    for n in (RIGHT0, LEFT0, RIGHT1, LEFT1):
        ring_copy(n).wait_send()
    partial_copy(0).wait_send()


def two_layers(tokens, layers, ep_size):
    halves, half_len, model_dim = tokens.shape
    operands = [tokens]
    anyspec = pl.BlockSpec(memory_space=pl.ANY)
    vmem = pl.BlockSpec(memory_space=pltpu.VMEM)
    specs = [anyspec]
    for params in layers:
        (attn_gain, w_query, w_key, w_value, w_out, moe_gain, w_router, routes, w_gate, w_up, w_down, shared_gate, shared_up, shared_down) = params
        heads, kv_heads, head_dim = w_query.shape[1], w_key.shape[1], w_query.shape[2]
        operands += [
            attn_gain, w_query, w_key, w_value, w_out.reshape(-1, model_dim),
            moe_gain, w_router.T, jnp.swapaxes(routes, 1, 2),
            w_gate, w_up, w_down, shared_gate, shared_up, shared_down,
        ]
        specs += [vmem, anyspec, anyspec, anyspec, anyspec, vmem, vmem, vmem] + [anyspec] * 6
    ff = w_gate.shape[2]
    top_k = routes.shape[-1]
    num_experts = w_gate.shape[0] * ep_size
    rows_half = 3 * half_len * top_k // num_experts
    block = (half_len, model_dim)
    dma = pltpu.SemaphoreType.DMA
    return pl.pallas_call(
        functools.partial(body, ep_size, heads, kv_heads, top_k, rows_half),
        out_shape=pltpu.VMEM(tokens.shape, BF16),
        in_specs=specs,
        out_specs=vmem,
        scratch_shapes=[
            pltpu.VMEM(w_query.shape, BF16),
            pltpu.VMEM(w_key.shape, BF16),
            pltpu.VMEM(w_value.shape, BF16),
            pltpu.VMEM((model_dim, (heads + 2 * kv_heads) * head_dim), BF16),
            pltpu.VMEM((heads * head_dim, model_dim), BF16),
            pltpu.VMEM((UNITS, 2) + block, BF16),
            pltpu.VMEM((UNITS, 2, 8, half_len), F32),
            pltpu.VMEM((2, ep_size, 8, half_len), F32),
            pltpu.VMEM((2, model_dim, ff), BF16),
            pltpu.VMEM((2, model_dim, ff), BF16),
            pltpu.VMEM((2, ff, model_dim), BF16),
            pltpu.VMEM((2, model_dim, CHUNK), BF16),
            pltpu.VMEM((2, model_dim, CHUNK), BF16),
            pltpu.VMEM((2, CHUNK, model_dim), BF16),
            pltpu.VMEM((2,) + block, F32),
            pltpu.VMEM((2, 2 * rows_half, model_dim), BF16),
            pltpu.VMEM((2 * rows_half, ff), BF16),
            pltpu.VMEM((1,) + block, F32),
            pltpu.VMEM((1,) + block, F32),
            pltpu.VMEM((1,) + block, F32),
            pltpu.VMEM((4,) + block, F32),
            pltpu.VMEM((6,) + block, F32),
            dma((5,)), dma((2, 3)), dma((2, 3)),
            dma((UNITS,)), dma((UNITS,)), dma((UNITS, 2)), dma((UNITS, 2)),
            dma((UNITS, 2)), dma((UNITS, 2)),
            dma((1,)), dma((1,)), dma((UNITS, 2)), dma((UNITS, 2)),
            pltpu.SemaphoreType.REGULAR((1,)),
        ],
        compiler_params=pltpu.CompilerParams(collective_id=0, has_side_effects=True, vmem_limit_bytes=62 * 2**20),
        name='two_layers',
    )(*operands)


def solution(mesh):
    ep_size = mesh.shape['ep']
    token_spec = P(('dp', 'ep'))
    layer_specs = (P(), P(), P(), P(), P(), P(), P(), token_spec, P('ep'), P('ep'), P('ep'), P(), P(), P())
    in_specs = (token_spec,) + layer_specs + layer_specs

    def local_step(tokens, *params):
        return two_layers(tokens, (params[:14], params[14:]), ep_size)

    return jax.shard_map(local_step, mesh=mesh, in_specs=in_specs, out_specs=token_spec, check_vma=False)
```

```python
import functools

import jax
import jax.numpy as jnp
from jax import lax
from jax.experimental import pallas as pl
from jax.experimental.pallas import tpu as pltpu
from jax.sharding import PartitionSpec as P

NORM_EPS = 1e-6
MESH = pl.DeviceIdType.MESH
F32 = jnp.float32
BF16 = jnp.bfloat16

LEFT0, OPP0, OPP1, RIGHT0, LEFT1, RIGHT1, OWN0, OWN1 = range(8)
UNITS = 8
CHUNK = 256
LAYERS = 2


def rms_norm(hidden, gain):
    inv_rms = lax.rsqrt(jnp.mean(hidden * hidden, axis=-1, keepdims=True) + NORM_EPS)
    return (hidden * inv_rms * gain).astype(BF16)


def body(
    ep_size, heads, kv_heads, top_k, rows_half,
    x_ref, *refs,
):
    layer_refs = (refs[:14], refs[14:28])
    (
        out_ref,
        qs, ks, vs, wqkv, wo, ub, mb, ms, wg, wu, wd, sg, su, sd, acc, xb, hb, keep, dsend, drecv, isend, rbuf,
        asem, wsem, shsem, fs, fr, uss, urs, mss, mrs, dss, drs, iss, irs, credit,
    ) = refs[28:]
    chips = ep_size // 2
    me = lax.axis_index('ep')
    chip, core = me // 2, me % 2
    other = 1 - core
    sib = 2 * chip + other
    left = 2 * ((chip + chips - 1) % chips) + core
    right = 2 * ((chip + 1) % chips) + core
    ff = wg.shape[2]
    model_dim = wg.shape[1]
    half_len = ub.shape[2]
    head_dim = model_dim // heads
    group = heads // kv_heads
    n_ff, n_out = ff // CHUNK, model_dim // CHUNK

    def remote(src, dst, send, recv, device):
        return pltpu.make_async_remote_copy(src_ref=src, dst_ref=dst, send_sem=send, recv_sem=recv, device_id={'ep': device}, device_id_type=MESH)

    def attention_weights(layer):
        return [
            pltpu.make_async_copy(ref, target, asem.at[i])
            for i, (ref, target) in enumerate(zip(layer_refs[layer][1:5], (qs, ks, vs, wo)))
        ]

    def place_weights():
        rows = model_dim // 8

        def place(r, carry):
            at = pl.ds(pl.multiple_of(r * rows, rows), rows)
            start = 0
            for staged in (qs, ks, vs):
                count = staged.shape[1]
                by_head = jnp.swapaxes(staged[at], 0, 1)
                for i in range(count):
                    wqkv[at, start + i * head_dim:start + (i + 1) * head_dim] = by_head[i]
                start += count * head_dim
            return carry

        lax.fori_loop(0, 8, place, 0, unroll=True)

    def shared_piece(layer, j, slot):
        sg_ref, su_ref, sd_ref = layer_refs[layer][11:14]
        cols = pl.ds(pl.multiple_of(j * CHUNK, CHUNK), CHUNK)
        return (
            pltpu.make_async_copy(sg_ref.at[:, cols], sg.at[slot], shsem.at[slot, 0]),
            pltpu.make_async_copy(su_ref.at[:, cols], su.at[slot], shsem.at[slot, 1]),
            pltpu.make_async_copy(sd_ref.at[cols, :], sd.at[slot], shsem.at[slot, 2]),
        )

    def expert_weights(layer, e):
        wg_ref, wu_ref, wd_ref = layer_refs[layer][8:11]
        return (
            pltpu.make_async_copy(wg_ref.at[e], wg.at[e], wsem.at[e, 0]),
            pltpu.make_async_copy(wu_ref.at[e], wu.at[e], wsem.at[e, 1]),
            pltpu.make_async_copy(wd_ref.at[e], wd.at[e], wsem.at[e, 2]),
        )

    def start_for(layer, make):
        for which in range(LAYERS):
            @pl.when(layer == which)
            def _():
                for copy in make(which):
                    copy.start()

    x_copy = pltpu.make_async_copy(x_ref, out_ref, asem.at[4])
    x_copy.start()
    for copy in attention_weights(0):
        copy.start()

    barrier = pltpu.get_barrier_semaphore()
    for step in range(1, ep_size):
        pl.semaphore_signal(barrier, inc=1, device_id={'ep': (me + step) % ep_size}, device_id_type=MESH)
    x_copy.wait()
    pl.semaphore_wait(barrier, ep_size - 1)

    def ring_u(src, slot, part, device):
        rows = pl.ds(part * (half_len // 2), half_len // 2)
        return remote(ub.at[src, core, rows], ub.at[slot, core, rows], uss.at[slot, part], urs.at[slot, part], device)

    def arrived(slot, *parts):
        for part in parts:
            ring_u(slot, slot, part, left).wait_recv()

    def partner_u(slot, part):
        rows = pl.ds(part * (half_len // 2), half_len // 2)
        return remote(ub.at[slot, core, rows], ub.at[slot, core, rows], fs.at[slot, part], fr.at[slot, part], sib)

    def hand_over(slot, *parts):
        for part in parts:
            partner_u(slot, part).start()

    def handed(slot):
        for part in range(2):
            rows = pl.ds(part * (half_len // 2), half_len // 2)
            remote(ub.at[slot, other, rows], ub.at[slot, other, rows], fs.at[slot, part], fr.at[slot, part], sib).wait_recv()

    hops = ((0, (OWN0, OWN1)), (1, (LEFT0, LEFT1)), (2, (OPP0, OPP1)), (3, (RIGHT0, RIGHT1)))

    def meta_sends(h):
        copies = []
        for hop, slots in hops:
            for flip in range(2):
                if hop == 0 and flip == 0:
                    continue
                dest = 2 * ((chip + hop) % chips) + (core + flip) % 2
                slot = slots[h]
                copies.append(remote(ms.at[h, dest], mb.at[slot, core], mss.at[slot, flip], mrs.at[slot, core], dest))
        return copies

    def partial_copy(slot):
        return remote(dsend.at[slot], drecv.at[slot], dss.at[slot], drs.at[slot], sib)

    def place_of(n):
        return n - 3 * (n // LEFT1)

    def ring_copy(n):
        device = right if n in (RIGHT0, RIGHT1) else left
        return remote(isend.at[place_of(n)], rbuf.at[n], iss.at[n, 0], irs.at[n, 0], device)

    def opposite_copy(n, part):
        rows = pl.ds(part * (half_len // 2), half_len // 2)
        return remote(isend.at[place_of(n), rows], rbuf.at[n, rows], iss.at[n, part], irs.at[n, part], (right, left)[part])

    def finish(h):
        from_left, from_right = RIGHT0 + (RIGHT1 - RIGHT0) * h, LEFT0 + (LEFT1 - LEFT0) * h
        for n in (from_left, from_right):
            remote(rbuf.at[n], rbuf.at[n], iss.at[n, 0], irs.at[n, 0], sib).wait_recv()
        out_ref[h] = (acc[h] + rbuf[from_left] + rbuf[from_right]).astype(BF16)

    def per_layer(layer, index):
        return jnp.where(layer == 0, layer_refs[0][index][...].astype(F32), layer_refs[1][index][...].astype(F32))

    def gain_of(layer, index):
        return per_layer(layer, index).reshape(1, model_dim)

    def attention_half(layer, h):
        normed = rms_norm(out_ref[h].astype(F32), gain_of(layer, 0))
        for j in range(wqkv.shape[1] // CHUNK):
            cols = slice(j * CHUNK, (j + 1) * CHUNK)
            hb[0:half_len, cols] = jnp.dot(normed, wqkv[:, cols], preferred_element_type=F32).astype(BF16)
        causal = lax.broadcasted_iota(jnp.int32, (half_len, half_len), 0) >= lax.broadcasted_iota(jnp.int32, (half_len, half_len), 1)
        for head in range(heads):
            kv = head // group
            query = hb[0:half_len, head * head_dim:(head + 1) * head_dim]
            keys = hb[0:half_len, (heads + kv) * head_dim:(heads + kv + 1) * head_dim]
            values = hb[0:half_len, (heads + kv_heads + kv) * head_dim:(heads + kv_heads + kv + 1) * head_dim]
            scores = lax.dot_general(query, keys, (((1,), (1,)), ((), ())), preferred_element_type=F32) * (head_dim ** -0.5)
            scores = jnp.where(causal, scores, -1e30)
            weights = jnp.exp(scores - jnp.max(scores, axis=-1, keepdims=True))
            probs = (weights / jnp.sum(weights, axis=-1, keepdims=True)).astype(BF16)
            xb[0, 0:half_len, head * head_dim:(head + 1) * head_dim] = jnp.dot(probs, values, preferred_element_type=F32).astype(BF16)
        for j in range(n_out):
            cols = slice(j * CHUNK, (j + 1) * CHUNK)
            projected = jnp.dot(xb[0, 0:half_len, :], wo[:, cols], preferred_element_type=F32)
            acc[h, :, cols] = (out_ref[h, :, cols].astype(F32) + projected).astype(BF16).astype(F32)
        ub[OWN0 + h, core] = rms_norm(acc[h], gain_of(layer, 5))

    def routing_half(layer, h):
        rows = ub[OWN0 + h, core]
        router = per_layer(layer, 6).astype(BF16)
        num_experts = router.shape[0]
        logits = lax.dot_general(router, rows, (((1,), (1,)), ((), ())), preferred_element_type=F32)
        picked = jnp.where(layer == 0, layer_refs[0][7][h], layer_refs[1][7][h])
        experts = lax.broadcasted_iota(jnp.int32, (num_experts, half_len), 0)
        chosen = picked[0:1, :] == experts
        for j in range(1, top_k):
            chosen = jnp.logical_or(chosen, picked[j:j + 1, :] == experts)
        masked = jnp.where(chosen, logits, -jnp.inf)
        weights = jnp.exp(masked - jnp.max(masked, axis=0, keepdims=True))
        gates = weights / jnp.sum(weights, axis=0, keepdims=True)
        before = (lax.broadcasted_iota(jnp.int32, (half_len, half_len), 0) < lax.broadcasted_iota(jnp.int32, (half_len, half_len), 1)).astype(BF16)
        place = jnp.dot(chosen.astype(F32).astype(BF16), before, preferred_element_type=F32)
        place = jnp.where(chosen, place, -1.0)
        for dest in range(ep_size):
            ms[h, dest, 0:2, :] = gates[2 * dest:2 * dest + 2, :]
            ms[h, dest, 2:4, :] = place[2 * dest:2 * dest + 2, :]
            ms[h, dest, 4:8, :] = jnp.zeros((4, half_len), F32)
        mb[OWN0 + h, core] = ms[h, me]

    def shared_expert(layer):
        def shared_step(j, carry):
            slot = j % 2

            @pl.when(j + 1 < n_ff)
            def _():
                start_for(layer, lambda which: shared_piece(which, j + 1, (j + 1) % 2))

            @pl.when(j == n_ff // 2 + 1)
            def _():
                arrived(LEFT0, 0)
                ring_u(LEFT0, OPP0, 0, right).start()
                ring_u(OWN1, LEFT1, 0, right).start()
                hand_over(LEFT0, 0)
                arrived(RIGHT0, 1)
                ring_u(RIGHT0, OPP0, 1, left).start()

            for copy in shared_piece(0, j, slot):
                copy.wait()
            for h, own in ((0, OWN0), (1, OWN1)):
                rows = ub[own, core]
                gate_act = jnp.dot(rows, sg[slot], preferred_element_type=F32)
                up_act = jnp.dot(rows, su[slot], preferred_element_type=F32)
                act = (jax.nn.silu(gate_act) * up_act).astype(BF16)
                acc[h] += jnp.dot(act, sd[slot], preferred_element_type=F32)
            return carry

        lax.fori_loop(0, n_ff, shared_step, 0)
        arrived(LEFT0, 1)
        hand_over(LEFT0, 1)
        arrived(RIGHT1, 1)
        ring_u(RIGHT1, OPP1, 1, left).start()
        ring_u(OWN0, RIGHT0, 0, left).start()
        ring_u(OWN1, RIGHT1, 0, left).start()

    def merge(layer, n):
        slot = 0
        partial_copy(slot).wait_recv()

        @pl.when(jnp.logical_or(n == OWN0, n == OWN1))
        def _():
            acc[n % 2] += keep[slot] + drecv[slot]

        for unit in (OPP0, OPP1, LEFT0):
            @pl.when(n == unit)
            def _():
                isend[place_of(unit)] = keep[slot] + drecv[slot]

        for unit, opp, part in ((RIGHT0, OPP0, 0), (LEFT1, OPP1, 1), (RIGHT1, OPP1, 0)):
            @pl.when(n == unit)
            def _():
                if unit == RIGHT0:
                    opposite_copy(OPP0, 1).wait_recv()
                    rest = slice(half_len // 2, half_len)
                    isend[place_of(LEFT0), rest] += rbuf[OPP0, rest]
                else:
                    for side in range(2):
                        opposite_copy(unit - LEFT1 + OPP0, side).wait_send()
                through = slice(part * (half_len // 2), (part + 1) * (half_len // 2))
                alone = slice((1 - part) * (half_len // 2), (2 - part) * (half_len // 2))
                isend[place_of(unit), alone] = keep[slot, alone] + drecv[slot, alone]
                if unit == RIGHT0:
                    ring_copy(LEFT0).start()
                opposite_copy(opp, part).wait_recv()
                isend[place_of(unit), through] = keep[slot, through] + drecv[slot, through] + rbuf[opp, through]

        @pl.when(UNITS * layer + n + 1 < UNITS * LAYERS)
        def _():
            pl.semaphore_signal(credit.at[slot], inc=1, device_id={'ep': sib}, device_id_type=MESH)

        for unit in (OPP0, OPP1):
            @pl.when(n == unit)
            def _():
                for side in range(2):
                    opposite_copy(unit, side).start()

        for unit in (RIGHT0, LEFT1, RIGHT1):
            @pl.when(n == unit)
            def _():
                ring_copy(unit).start()

    def unit_step(layer, n):
        @pl.when(n == LEFT0)
        def _():
            for copy in expert_weights(0, 0)[:2]:
                copy.wait()

        @pl.when(n == OPP0)
        def _():
            arrived(LEFT1, 0)
            ring_u(LEFT1, OPP1, 0, right).start()
            ring_u(OWN1, LEFT1, 1, right).start()

        for part, kk in ((1, core), (0, other)):
            if part == 0:
                handed(n)

            @pl.when(jnp.logical_or(jnp.logical_and(n != OWN0, n != OWN1), kk != core))
            def _():
                remote(mb.at[n, kk], mb.at[n, kk], mss.at[n, 0], mrs.at[n, kk], sib).wait_recv()

            picks = []
            for e in range(2):
                place = mb[n, kk, 2 + e:3 + e, :].astype(jnp.int32)
                picks.append((place == lax.broadcasted_iota(jnp.int32, (rows_half, half_len), 0)).astype(BF16))
            pick = jnp.concatenate(picks, axis=0)
            for j in range(n_out):
                cols = slice(j * CHUNK, (j + 1) * CHUNK)
                both = jnp.dot(pick, ub[n, kk, :, cols], preferred_element_type=F32).astype(BF16)
                for e in range(2):
                    xb[e, part * rows_half:(part + 1) * rows_half, cols] = both[e * rows_half:(e + 1) * rows_half]

        def up(e, pieces):
            rows = xb[e]
            for j in pieces:
                cols = slice(j * CHUNK, (j + 1) * CHUNK)
                gate_act = jnp.dot(rows, wg[e, :, cols], preferred_element_type=F32)
                up_act = jnp.dot(rows, wu[e, :, cols], preferred_element_type=F32)
                hb[:, cols] = (jax.nn.silu(gate_act) * up_act).astype(BF16)

        def down(e):
            for j in range(n_out):
                cols = slice(j * CHUNK, (j + 1) * CHUNK)
                xb[e, :, cols] = jnp.dot(hb[...], wd[e, :, cols], preferred_element_type=F32).astype(BF16)

        up(0, range(n_ff // 2 + 1))

        @pl.when(n == LEFT0)
        def _():
            for copy in expert_weights(0, 0)[2:] + expert_weights(0, 1):
                copy.wait()

        @pl.when(n == OPP1)
        def _():
            arrived(LEFT1, 1)
            arrived(RIGHT0, 0)
            arrived(RIGHT1, 0)
            for slot in (RIGHT0, LEFT1, RIGHT1):
                hand_over(slot, 0, 1)

        @pl.when(n == RIGHT0)
        def _():
            for slot in range(UNITS):
                for part in range(2):
                    partner_u(slot, part).wait_send()
            for slot in range(LEFT0, OWN0):
                for part in range(2):
                    ring_u(slot, slot, part, right).wait_send()
            for h in range(2):
                for copy in meta_sends(h):
                    copy.wait_send()

        @pl.when(n > 0)
        def _():
            merge(layer, n - 1)

        up(0, range(n_ff // 2 + 1, n_ff))
        down(0)
        up(1, range(n_ff))

        @pl.when(n == LEFT0)
        def _():
            arrived(OPP0, 0, 1)
            hand_over(OPP0, 0, 1)

        @pl.when(n == OPP0)
        def _():
            arrived(OPP1, 0, 1)
            hand_over(OPP1, 0, 1)

        slot = 0

        @pl.when(UNITS * layer + n >= 1)
        def _():
            partial_copy(slot).wait_send()
            pl.semaphore_wait(credit.at[slot], 1)

        down(1)

        for part, kk in ((0, other), (1, core)):
            columns = jnp.transpose(mb[n, kk])
            picks = []
            for e in range(2):
                place = columns[:, 2 + e:3 + e].astype(jnp.int32)
                picks.append((place == lax.broadcasted_iota(jnp.int32, (half_len, rows_half), 1)).astype(BF16))
            target = dsend if part == 0 else keep
            for j in range(n_out):
                cols = slice(j * CHUNK, (j + 1) * CHUNK)
                total = None
                for e in range(2):
                    row = jnp.dot(picks[e], xb[e, part * rows_half:(part + 1) * rows_half, cols], preferred_element_type=F32)
                    term = columns[:, e:e + 1] * row
                    total = term if total is None else total + term
                target[slot, :, cols] = total
        partial_copy(slot).start()

    def layer_step(layer, carry):
        start_for(layer, lambda which: shared_piece(which, 0, 0))
        for e in range(2):
            start_for(layer, lambda which: expert_weights(which, e))

        def half_step(h, carry):
            @pl.when(layer > 0)
            def _():
                finish(h)

            @pl.when(h == 0)
            def _():
                *projections, out_weights = attention_weights(0)
                for copy in projections:
                    copy.wait()
                place_weights()
                out_weights.wait()

            attention_half(layer, h)
            routing_half(layer, h)

            @pl.when(h == 0)
            def _():
                ring_u(OWN0, LEFT0, 0, right).start()
                ring_u(OWN0, RIGHT0, 1, left).start()
                ring_u(OWN0, LEFT0, 1, right).start()
                hand_over(OWN0, 0, 1)
                for copy in meta_sends(0):
                    copy.start()

            @pl.when(h == 1)
            def _():
                ring_u(OWN1, RIGHT1, 1, left).start()
                hand_over(OWN1, 0, 1)
                for copy in meta_sends(1):
                    copy.start()
            return carry

        lax.fori_loop(0, 2, half_step, 0)

        @pl.when(layer + 1 < LAYERS)
        def _():
            for copy in attention_weights(1):
                copy.start()

        @pl.when(layer > 0)
        def _():
            for n in (RIGHT0, LEFT0, RIGHT1, LEFT1):
                ring_copy(n).wait_send()

        def step(n, carry):
            unit_step(layer, n)
            return carry

        shared_expert(layer)
        lax.fori_loop(0, UNITS, step, 0)
        merge(layer, OWN1)
        return carry

    lax.fori_loop(0, LAYERS, layer_step, 0)
    for h in range(2):
        finish(h)
    for n in (RIGHT0, LEFT0, RIGHT1, LEFT1):
        ring_copy(n).wait_send()
    partial_copy(0).wait_send()


def two_layers(tokens, layers, ep_size):
    halves, half_len, model_dim = tokens.shape
    operands = [tokens]
    anyspec = pl.BlockSpec(memory_space=pl.ANY)
    vmem = pl.BlockSpec(memory_space=pltpu.VMEM)
    specs = [anyspec]
    for params in layers:
        (attn_gain, w_query, w_key, w_value, w_out, moe_gain, w_router, routes, w_gate, w_up, w_down, shared_gate, shared_up, shared_down) = params
        heads, kv_heads, head_dim = w_query.shape[1], w_key.shape[1], w_query.shape[2]
        operands += [
            attn_gain, w_query, w_key, w_value, w_out.reshape(-1, model_dim),
            moe_gain, w_router.T, jnp.swapaxes(routes, 1, 2),
            w_gate, w_up, w_down, shared_gate, shared_up, shared_down,
        ]
        specs += [vmem, anyspec, anyspec, anyspec, anyspec, vmem, vmem, vmem] + [anyspec] * 6
    ff = w_gate.shape[2]
    top_k = routes.shape[-1]
    num_experts = w_gate.shape[0] * ep_size
    rows_half = 3 * half_len * top_k // num_experts
    block = (half_len, model_dim)
    dma = pltpu.SemaphoreType.DMA
    return pl.pallas_call(
        functools.partial(body, ep_size, heads, kv_heads, top_k, rows_half),
        out_shape=pltpu.VMEM(tokens.shape, BF16),
        in_specs=specs,
        out_specs=vmem,
        scratch_shapes=[
            pltpu.VMEM(w_query.shape, BF16),
            pltpu.VMEM(w_key.shape, BF16),
            pltpu.VMEM(w_value.shape, BF16),
            pltpu.VMEM((model_dim, (heads + 2 * kv_heads) * head_dim), BF16),
            pltpu.VMEM((heads * head_dim, model_dim), BF16),
            pltpu.VMEM((UNITS, 2) + block, BF16),
            pltpu.VMEM((UNITS, 2, 8, half_len), F32),
            pltpu.VMEM((2, ep_size, 8, half_len), F32),
            pltpu.VMEM((2, model_dim, ff), BF16),
            pltpu.VMEM((2, model_dim, ff), BF16),
            pltpu.VMEM((2, ff, model_dim), BF16),
            pltpu.VMEM((2, model_dim, CHUNK), BF16),
            pltpu.VMEM((2, model_dim, CHUNK), BF16),
            pltpu.VMEM((2, CHUNK, model_dim), BF16),
            pltpu.VMEM((2,) + block, F32),
            pltpu.VMEM((2, 2 * rows_half, model_dim), BF16),
            pltpu.VMEM((2 * rows_half, ff), BF16),
            pltpu.VMEM((1,) + block, F32),
            pltpu.VMEM((1,) + block, F32),
            pltpu.VMEM((1,) + block, F32),
            pltpu.VMEM((4,) + block, F32),
            pltpu.VMEM((6,) + block, F32),
            dma((5,)), dma((2, 3)), dma((2, 3)),
            dma((UNITS, 2)), dma((UNITS, 2)), dma((UNITS, 2)), dma((UNITS, 2)),
            dma((UNITS, 2)), dma((UNITS, 2)),
            dma((1,)), dma((1,)), dma((UNITS, 2)), dma((UNITS, 2)),
            pltpu.SemaphoreType.REGULAR((1,)),
        ],
        compiler_params=pltpu.CompilerParams(collective_id=0, has_side_effects=True, vmem_limit_bytes=62 * 2**20),
        name='two_layers',
    )(*operands)


def solution(mesh):
    ep_size = mesh.shape['ep']
    token_spec = P(('dp', 'ep'))
    layer_specs = (P(), P(), P(), P(), P(), P(), P(), token_spec, P('ep'), P('ep'), P('ep'), P(), P(), P())
    in_specs = (token_spec,) + layer_specs + layer_specs

    def local_step(tokens, *params):
        return two_layers(tokens, (params[:14], params[14:]), ep_size)

    return jax.shard_map(local_step, mesh=mesh, in_specs=in_specs, out_specs=token_spec, check_vma=False)
```
